32 devices in a mesh: gx: 4 (over y, x), gy: 4 (over z), gz: 2 (over core).
Axes of the slice: x: 2, y: 2, z: 4, core: 2. Of those that a mesh axis runs over, the one named last changes fastest.
Arguments:
- densities: float32 [7, 64, 128, 512], P(None, 'gz', 'gy', 'gx'), may hold values from -6 to 6
- residuals: float32 [7, 64, 128, 512], P(None, 'gz', 'gy', 'gx'), may hold values from -320 to 320
Outputs:
- new_density: float32 [64, 128, 512], P('gz', 'gy', 'gx')
- weights: float32 [7], replicated
The draws below stay inside these ranges and needn't reach their ends.
All inputs are finite; a program needn't handle non-finite values.
Results may differ from the reference program's by a relative error of at most 0.000087.
Values sent between devices are 32-bit elements; how exact they have to be, the bound alone decides.
A program may use at most 64 MiB of HBM per device.

```python
import math
import jax
import jax.numpy as jnp
from jax import lax

HIST1 = 7
SWEEPS = 3
NX = 512
NY = 128
NZ = 64


def draw_residuals(key, part):
    keys = jax.random.split(jax.random.fold_in(key, 11), 4)
    base = jnp.clip(jax.random.normal(keys[0], (1, NZ, NY, NX), jnp.float32), -6.0, 6.0)
    zpos = jnp.arange(NZ, dtype=jnp.float32) / NZ
    rows = jnp.exp(jax.random.uniform(keys[3], (1, 1, NY, 1), jnp.float32, 0.0, math.log(3.0)))
    noise = 0.7 * jnp.clip(jax.random.normal(keys[1], (HIST1, NZ, NY, NX), jnp.float32), -6.0, 6.0)
    mixing = jax.random.uniform(keys[2], (HIST1, 1, 1, 1), jnp.float32, 0.5, 1.0)
    ramp = jnp.power(10.0, zpos)
    return (mixing * base + noise) * ramp.reshape(1, NZ, 1, 1) * rows


def levels(own_key, extent, pieces, low, top_value):
    loudness, own = 1.0, jax.random.fold_in(own_key, 6)
    for axis_at, blocks in pieces:
        heights = jnp.exp(jax.random.uniform(jax.random.fold_in(own, axis_at), (blocks,), jnp.float32, low / len(pieces), top_value / len(pieces)))
        loudness = loudness * jnp.repeat(heights, extent[axis_at] // blocks).reshape([-1 if axis == axis_at else 1 for axis in range(len(extent))])
    return loudness


def scatter_about(own_key, dims, spread, bound, shards=(), held_as=jnp.bfloat16):
    array = spread * jax.random.normal(own_key, dims, jnp.float32)
    if shards:
        array = array * levels(own_key, dims, shards, -0.22, 0.18)
    return jnp.clip(array, -bound, bound).astype(held_as)


def setup_inputs(seed: int = 0) -> dict:
    seeds = jax.random.split(jax.random.key(seed), 3)
    return {
        "densities": scatter_about(seeds[0], (HIST1, NZ, NY, NX), 1.0, 6.0, ((1, 2), (2, 4), (3, 4)), jnp.float32),
        "residuals": draw_residuals(jax.random.fold_in(seeds[2], 71), 0),
    }


shift_value = 0.15
mix_amount = 0.7

def sweep_weights():
    diag_value = 6.0 + shift_value
    upper = (shift_value + 12.0) / diag_value
    lower = upper / 3.0
    return [1.0 / ((upper + lower) / 2.0 + (upper - lower) / 2.0 * math.cos(math.pi * (2 * k - 1) / (2 * SWEEPS))) for k in range(1, SWEEPS + 1)]

def neighbours(field):
    total = jnp.roll(field, 1, 0) + jnp.roll(field, -1, 0)
    total = total + jnp.roll(field, 1, 1) + jnp.roll(field, -1, 1)
    return total + jnp.roll(field, 1, 2) + jnp.roll(field, -1, 2)

def reference(densities, residuals):
    flat = residuals.reshape(HIST1, -1)
    gram = jnp.dot(flat.astype(jnp.float32), flat.T.astype(jnp.float32), precision=lax.Precision.HIGHEST, preferred_element_type=jnp.float32)
    factor = jnp.linalg.cholesky(gram)
    ones_column = jnp.ones((HIST1, 1), jnp.float32)
    middle = lax.linalg.triangular_solve(factor, ones_column, left_side=True, lower=True)
    solved = lax.linalg.triangular_solve(factor, middle, left_side=True, lower=True, transpose_a=True)[:, 0]
    weights = solved / jnp.sum(solved)
    blended = jnp.tensordot(weights, densities, axes=1, precision=lax.Precision.HIGHEST)
    combined = jnp.tensordot(weights, residuals, axes=1, precision=lax.Precision.HIGHEST)
    diag_value = 6.0 + shift_value
    omegas = sweep_weights()
    rhs = 6.0 * combined - neighbours(combined)
    iterate = omegas[0] * rhs / diag_value
    for position in range(1, SWEEPS):
        iterate = iterate + omegas[position] * (rhs - diag_value * iterate + neighbours(iterate)) / diag_value
    return (blended + mix_amount * iterate, weights)
```

```python
import functools
import math

import jax
import jax.numpy as jnp
from jax import lax
from jax.experimental import pallas as pl
from jax.experimental.pallas import tpu as pltpu
from jax.sharding import PartitionSpec as P

MESH = pl.DeviceIdType.MESH
SWEEPS = 3
SUB = 8
UNROLL = 4
shift_value = 0.15
mix_amount = 0.7
AXES = ("gx", "gy", "gz")


def sweep_weights():
    diag_value = 6.0 + shift_value
    upper = (shift_value + 12.0) / diag_value
    lower = upper / 3.0
    return [
        1.0
        / (
            (upper + lower) / 2.0
            + (upper - lower) / 2.0 * math.cos(math.pi * (2 * k - 1) / (2 * SWEEPS))
        )
        for k in range(1, SWEEPS + 1)
    ]


def sweep_factors():
    diag_value = 6.0 + shift_value
    w1, w2, w3 = sweep_weights()
    alpha = ((1.0 - w2) * w1 + w2) / diag_value
    beta = w1 * w2 / (diag_value * diag_value)
    return alpha, beta, mix_amount * (1.0 - w3), mix_amount * w3 / diag_value


def neighbour_polynomial():
    alpha, beta, keep, step = sweep_factors()
    q0 = keep * alpha + step
    q1 = keep * beta + step * alpha
    q2 = step * beta
    return 6.0 * q0, 6.0 * q1 - q0, 6.0 * q2 - q1, -q2


def kernel(
    counts, dims, chunks,
    res, den, base, xc, yc, wout,
    held, dens, slots, comb, rhs, it, raw, pack, land, ybuf, yland,
    in_sem, den_sem, gsend, grecv, zsend, zrecv, ysend, yrecv, xsend, xrecv, csend, crecv,
):
    count, nz, ny, nx = dims
    cx, cy, cz = counts
    total_devices = cx * cy * cz
    h = SWEEPS
    ze = nz + 2 * h
    zp = yland.shape[1] // h
    tiles = ny // SUB
    ix, iy, iz = (lax.axis_index(a) for a in AXES)
    me = (ix * cy + iy) * cz + iz

    def near(dx, dy, dz):
        return (
            lax.rem(ix + dx + cx, cx),
            lax.rem(iy + dy + cy, cy),
            lax.rem(iz + dz + cz, cz),
        )

    per = nz // chunks
    loads = []
    for c in range(chunks):
        cp = pltpu.make_async_copy(
            res.at[:, pl.ds(c * per, per)], held.at[:, pl.ds(h + c * per, per)], in_sem.at[c]
        )
        cp.start()
        loads.append(cp)

    barrier = pltpu.get_barrier_semaphore()

    offsets = [
        (dx, dy, dz) for dx in range(cx) for dy in range(cy) for dz in range(cz) if dx or dy or dz
    ]
    offsets.sort(key=lambda o: -sum(min(d, c - d) for d, c in zip(o, counts)))
    gx = [lax.rem(ix + d, cx) for d in range(cx)]
    gy = [lax.rem(iy + d, cy) for d in range(cy)]
    gz = [lax.rem(iz + d, cz) for d in range(cz)]
    for dx, dy, dz in offsets:
        pl.semaphore_signal(
            barrier, inc=1, device_id=(gx[dx], gy[dy], gz[dz]), device_id_type=MESH
        )

    pairs = [(i, j) for i in range(count) for j in range(i, count)]
    accs = tuple(jnp.zeros((SUB, nx), jnp.float32) for _ in pairs)
    den_load = pltpu.make_async_copy(den, dens, den_sem)
    for c in range(chunks):
        loads[c].wait()
        if c == chunks - 1:
            den_load.start()

        def gram_step(z, accs):
            accs = list(accs)
            for t in range(tiles):
                v = [held[i, z, t * SUB:(t + 1) * SUB, :] for i in range(count)]
                for p, (i, j) in enumerate(pairs):
                    accs[p] = accs[p] + v[i] * v[j]
            return tuple(accs)

        accs = lax.fori_loop(h + c * per, h + (c + 1) * per, gram_step, accs)
    lane = lax.broadcasted_iota(jnp.int32, (SUB, nx), 1)
    packed = jnp.zeros((SUB, nx), jnp.float32)
    for p in range(len(pairs)):
        packed = jnp.where(lane == p, jnp.sum(accs[p], axis=1, keepdims=True), packed)
    slots[pl.ds(me, 1)] = jnp.sum(packed, axis=0, keepdims=True).reshape(1, 1, nx)

    pl.semaphore_wait(barrier, total_devices - 1)

    def gram_copy(k, slot):
        dx, dy, dz = offsets[k]
        return pltpu.make_async_remote_copy(
            src_ref=slots.at[me],
            dst_ref=slots.at[slot],
            send_sem=gsend.at[k],
            recv_sem=grecv.at[k],
            device_id=(gx[dx], gy[dy], gz[dz]),
            device_id_type=MESH,
        )

    for k in range(len(offsets)):
        gram_copy(k, me).start()

    zcopies = []
    for k, (start, dest, dz) in enumerate(((h, nz + h, -1), (nz, 0, 1))):
        cp = pltpu.make_async_remote_copy(
            src_ref=held.at[:, pl.ds(start, h)],
            dst_ref=held.at[:, pl.ds(dest, h)],
            send_sem=zsend.at[k],
            recv_sem=zrecv.at[k],
            device_id=near(0, 0, dz),
            device_id_type=MESH,
        )
        cp.start()
        zcopies.append(cp)

    third = lane // h

    def gather_faces(rows, fresh):
        @pl.loop(0, count)
        def _(i):
            for t in range(tiles):
                span = slice(t * SUB, (t + 1) * SUB)
                if fresh:
                    head = jnp.zeros((SUB, nx), jnp.float32)
                    tail = head
                else:
                    head, tail = raw[i, 0, span, :], raw[i, 1, span, :]
                for z in rows:
                    v = pltpu.roll(held[i, z, span, :], h * z + h, 1)
                    head = jnp.where(third == z + 1, v, head)
                    tail = jnp.where(third == z, v, tail)
                raw[i, 0, span, :] = head
                raw[i, 1, span, :] = tail

    gather_faces(range(h, nz + h), True)

    for p in range(h, SUB):
        yc[p * zp:(p + 1) * zp, :] = jnp.zeros((zp, nx), jnp.float32)
        mirror = 2 * SUB - 1 - p
        yc[mirror * zp:(mirror + 1) * zp, :] = jnp.zeros((zp, nx), jnp.float32)

    for cp in zcopies:
        cp.wait()
    gather_faces((*range(h), *range(nz + h, ze)), False)

    for k, (dx, dy, dz) in enumerate(offsets):
        source = (gx[-dx % cx] * cy + gy[-dy % cy]) * cz + gz[-dz % cz]
        gram_copy(k, source).wait_recv()

    total = jnp.sum(slots[...], axis=0)

    g = {}
    for p, (i, j) in enumerate(pairs):
        g[i, j] = jnp.broadcast_to(total[:, p:p + 1], (SUB, nx))
    b = [jnp.ones((SUB, nx), jnp.float32) for _ in range(count)]
    inv = []
    for k in range(count):
        inv.append(1.0 / g[k, k])
        for i in range(k + 1, count):
            f = g[k, i] * inv[k]
            for j in range(i, count):
                g[i, j] = g[i, j] - f * g[k, j]
            b[i] = b[i] - f * b[k]
    solved = [None] * count
    for k in reversed(range(count)):
        s = b[k]
        for j in range(k + 1, count):
            s = s - g[k, j] * solved[j]
        solved[k] = s * inv[k]
    norm = solved[0]
    for k in range(1, count):
        norm = norm + solved[k]
    weights = [s / norm for s in solved]

    for k in range(2):
        for t in range(tiles):
            span = slice(t * SUB, (t + 1) * SUB)
            s = weights[0] * raw[0, k, span, :]
            for i in range(1, count):
                s = s + weights[i] * raw[i, k, span, :]
            pack[k, span, :] = s

    copies = []

    def send(source, target, send_sem, recv_sem, dx, dy):
        cp = pltpu.make_async_remote_copy(
            src_ref=source,
            dst_ref=target,
            send_sem=send_sem,
            recv_sem=recv_sem,
            device_id=near(dx, dy, 0),
            device_id_type=MESH,
        )
        cp.start()
        copies.append(cp)

    for k, dx in enumerate((-1, 1)):
        side = land.at[1 - k]
        send(
            pack.at[k, pl.ds(ny - SUB, SUB)], side.at[pl.ds(0, SUB)],
            csend.at[k, 0], crecv.at[k, 0], dx, 1,
        )
        send(
            pack.at[k, pl.ds(0, SUB)], side.at[pl.ds(ny + SUB, SUB)],
            csend.at[k, 1], crecv.at[k, 1], dx, -1,
        )
    for k, dx in enumerate((-1, 1)):
        send(pack.at[k], land.at[1 - k, pl.ds(SUB, ny)], xsend.at[k], xrecv.at[k], dx, 0)

    def combine(z, t):
        span = slice(t * SUB, (t + 1) * SUB)
        s = weights[0] * held[0, z, span, :]
        for i in range(1, count):
            s = s + weights[i] * held[i, z, span, :]
        comb[z, span, :] = s
        return s

    @pl.loop(0, ze // 2)
    def _(half):
        for r in range(2):
            z = half * 2 + r
            for k, t in enumerate((0, tiles - 1)):
                ybuf[pl.ds(k * SUB * zp + z, SUB, stride=zp), :] = combine(z, t)

    for k, (start, dy) in enumerate(((0, -1), ((2 * SUB - h) * zp, 1))):
        send(
            ybuf.at[pl.ds(start, h * zp)], yland.at[1 - k],
            ysend.at[k], yrecv.at[k], 0, dy,
        )

    @pl.loop(0, ze // 2)
    def _(half):
        for r in range(2):
            for t in range(1, tiles - 1):
                combine(half * 2 + r, t)

    row = jnp.zeros((SUB, nx), jnp.float32)
    for k in range(count):
        row = jnp.where(lane == k, weights[k], row)
    wout[...] = row[0:1, :count]

    def around(f, z):
        v = f[z]
        total = pltpu.roll(v, 1, 1) + pltpu.roll(v, nx - 1, 1)
        total = total + (pltpu.roll(v, 1, 0) + pltpu.roll(v, ny - 1, 0))
        return v, total + (f[z - 1] + f[z + 1])

    def planes(start, stop, unroll):
        steps = (stop - start) // unroll

        def wrap(body):
            @pl.loop(0, steps)
            def _(block):
                for r in range(unroll):
                    body(start + block * unroll + r)

            for z in range(start + steps * unroll, stop):
                body(z)
            return body

        return wrap

    alpha, beta, keep, step = sweep_factors()

    @planes(1, ze - 1, UNROLL)
    def _(z):
        v, total = around(comb, z)
        rhs[z] = 6.0 * v - total

    @planes(2, ze - 2, UNROLL)
    def _(z):
        v, total = around(rhs, z)
        it[z] = alpha * v + beta * total

    den_load.wait()

    @planes(h, nz + h, UNROLL)
    def _(z):
        v, total = around(it, z)
        u = keep * v + step * (rhs[z] + total)
        for t in range(tiles):
            span = slice(t * SUB, (t + 1) * SUB)
            s = weights[0] * dens[0, z - h, span, :]
            for i in range(1, count):
                s = s + weights[i] * dens[i, z - h, span, :]
            base[z - h, span, :] = s + u[span, :]

    for cp in copies:
        cp.wait()

    _, c1, c2, c3 = neighbour_polynomial()

    def by_distance(first, second, square):
        near_by = (c1 + 3.0 * c3) * first + (2.0 * c2) * second + (3.0 * c3) * square
        return near_by, c2 * first + (3.0 * c3) * second

    wide = ny + 2 * SUB
    inside = slice(SUB, SUB + ny)
    column = lax.broadcasted_iota(jnp.int32, (ny, nx), 1)
    place = column % h

    def plane_sum(d):
        total = pltpu.roll(d, h, 1) + pltpu.roll(d, nx - h, 1)
        return total + (pltpu.roll(d, 1, 0) + pltpu.roll(d, wide - 1, 0))

    sides = []
    for s in range(2):
        own = pack[1 - s]
        d = land[s] - jnp.concatenate([own[ny - SUB:], own, own[:SUB]], axis=0)
        m = plane_sum(d)
        mm = plane_sum(m)
        a1, a2 = by_distance(d[inside], m[inside], mm[inside])
        a3 = c3 * d[inside]
        if s == 0:
            a1, a2, a3 = (pltpu.roll(a, k + 1, 1) for k, a in enumerate((a1, a2, a3)))
            depth = place
        else:
            a1, a2, a3 = (pltpu.roll(a, nx - k - 1, 1) for k, a in enumerate((a1, a2, a3)))
            depth = (h - 1) - place
        sides.append(
            jnp.where(depth == 0, a1, 0.0) + jnp.where(depth <= 1, a2, 0.0) + a3
        )
    even = (column // h) % 2 == 0
    xc[0] = jnp.where(even, sides[1], sides[0])
    xc[1] = jnp.where(even, sides[0], sides[1])

    along = lax.broadcasted_iota(jnp.int32, (zp, nx), 1)
    at_first, at_last = along == 0, along == nx - 1

    def face_sum(d):
        total = jnp.where(at_first, 0.0, pltpu.roll(d, 1, 1))
        total = total + jnp.where(at_last, 0.0, pltpu.roll(d, nx - 1, 1))
        return total + (pltpu.roll(d, 1, 0) + pltpu.roll(d, zp - 1, 0))

    for s in range(2):
        ds = []
        for k in range(h):
            p = h - 1 - k if s == 0 else k
            q = 2 * SUB - 1 - k if s == 0 else k
            ds.append(yland[s, p * zp:(p + 1) * zp, :] - ybuf[q * zp:(q + 1) * zp, :])
        m = face_sum(ds[0])
        mm = face_sum(m) + jnp.where(at_first | at_last, ds[0], 0.0)
        near_1, near_2 = by_distance(ds[0], m, mm)
        rows = [
            near_1 + (c2 * ds[1] + (3.0 * c3) * face_sum(ds[1])) + c3 * ds[2],
            near_2 + c3 * ds[1],
            c3 * ds[0],
        ]
        for j, r in enumerate(rows):
            p = j if s == 0 else 2 * SUB - 1 - j
            yc[p * zp:(p + 1) * zp, :] = r

    for k in range(len(offsets)):
        gram_copy(k, me).wait_send()


def finish(base, xc, yc, weights, out, wout, stage, sem, wsem):
    nz, ny, nx = base.shape
    h = SWEEPS
    zp = yc.shape[0] // (2 * SUB)
    tiles = ny // SUB
    pieces = sem.shape[0]
    per = nz // pieces
    wcopy = pltpu.make_async_copy(weights, wout, wsem)
    wcopy.start()
    lane = lax.broadcasted_iota(jnp.int32, (SUB, nx), 1)
    edge = (lane < h) | (lane >= nx - h)
    copies = []
    for c in range(pieces):
        for z in range(c * per, (c + 1) * per):
            e = z + h
            for t in range(tiles):
                span = slice(t * SUB, (t + 1) * SUB)
                v = pltpu.roll(xc[e % 2, span, :], (-(h * e + h)) % nx, 1)
                v = base[z, span, :] + jnp.where(edge, v, 0.0)
                if t == 0:
                    v = v + yc[pl.ds(e, SUB, stride=zp), :]
                if t == tiles - 1:
                    v = v + yc[pl.ds(SUB * zp + e, SUB, stride=zp), :]
                stage[z, span, :] = v
        part = pl.ds(c * per, per)
        cp = pltpu.make_async_copy(stage.at[part], out.at[part], sem.at[c])
        cp.start()
        copies.append(cp)
    for cp in copies:
        cp.wait()
    wcopy.wait()


def on_device(counts, densities, residuals):
    dims = residuals.shape
    count, nz, ny, nx = dims
    h = SWEEPS
    ze = nz + 2 * h
    zp = pl.cdiv(ze, SUB) * SUB
    n = counts[0] * counts[1] * counts[2]
    chunks = 8
    tiles = ny // SUB
    assert tiles >= 2 and h * (ze + 1) <= nx
    dma = pltpu.SemaphoreType.DMA
    f32 = jnp.float32
    field = pltpu.VMEM((ze, ny, nx), f32)

    any_spec = pl.BlockSpec(memory_space=pl.ANY)
    vmem = pl.BlockSpec(memory_space=pltpu.VMEM)
    parts = pl.pallas_call(
        functools.partial(kernel, counts, dims, chunks),
        out_shape=(
            pltpu.VMEM((nz, ny, nx), f32),
            pltpu.VMEM((2, ny, nx), f32),
            pltpu.VMEM((2 * SUB * zp, nx), f32),
            pltpu.VMEM((1, count), f32),
        ),
        in_specs=[any_spec, any_spec],
        out_specs=(vmem, vmem, vmem, vmem),
        scratch_shapes=[
            pltpu.VMEM((count, ze, ny, nx), f32),
            pltpu.VMEM(dims, f32),
            pltpu.VMEM((n, 1, nx), f32),
            field, field, field,
            pltpu.VMEM((count, 2, ny, nx), f32),
            pltpu.VMEM((2, ny, nx), f32),
            pltpu.VMEM((2, ny + 2 * SUB, nx), f32),
            pltpu.VMEM((2 * SUB * zp, nx), f32),
            pltpu.VMEM((2, h * zp, nx), f32),
            dma((chunks,)), dma(()), dma((n,)), dma((n,)),
            dma((2,)), dma((2,)), dma((2,)), dma((2,)), dma((2,)), dma((2,)), dma((2, 2)), dma((2, 2)),
        ],
        compiler_params=pltpu.CompilerParams(
            collective_id=0, has_side_effects=True, vmem_limit_bytes=56 * 1024 * 1024
        ),
    )(residuals, densities)
    new_density, weights = pl.pallas_call(
        finish,
        out_shape=(
            jax.ShapeDtypeStruct((nz, ny, nx), f32),
            jax.ShapeDtypeStruct((1, count), f32),
        ),
        in_specs=[vmem, vmem, vmem, vmem],
        out_specs=(any_spec, any_spec),
        scratch_shapes=[pltpu.VMEM((nz, ny, nx), f32), dma((8,)), dma(())],
        compiler_params=pltpu.CompilerParams(vmem_limit_bytes=4 * 1024 * 1024),
    )(*parts)
    return new_density, weights.reshape(count)


def solution(mesh):
    counts = tuple(mesh.shape[a] for a in AXES)
    placed = (P(None, "gz", "gy", "gx"), P(None, "gz", "gy", "gx"))
    return jax.shard_map(
        functools.partial(on_device, counts),
        mesh=mesh,
        in_specs=placed,
        out_specs=(P("gz", "gy", "gx"), P()),
        check_vma=False,
    )
```

```python
import functools
import math

import jax
import jax.numpy as jnp
from jax import lax
from jax.experimental import pallas as pl
from jax.experimental.pallas import tpu as pltpu
from jax.sharding import PartitionSpec as P

MESH = pl.DeviceIdType.MESH
SWEEPS = 3
SUB = 8
UNROLL = 4
shift_value = 0.15
mix_amount = 0.7
AXES = ("gx", "gy", "gz")


def sweep_weights():
    diag_value = 6.0 + shift_value
    upper = (shift_value + 12.0) / diag_value
    lower = upper / 3.0
    return [
        1.0
        / (
            (upper + lower) / 2.0
            + (upper - lower) / 2.0 * math.cos(math.pi * (2 * k - 1) / (2 * SWEEPS))
        )
        for k in range(1, SWEEPS + 1)
    ]


def sweep_factors():
    diag_value = 6.0 + shift_value
    w1, w2, w3 = sweep_weights()
    alpha = ((1.0 - w2) * w1 + w2) / diag_value
    beta = w1 * w2 / (diag_value * diag_value)
    return alpha, beta, mix_amount * (1.0 - w3), mix_amount * w3 / diag_value


def neighbour_polynomial():
    alpha, beta, keep, step = sweep_factors()
    q0 = keep * alpha + step
    q1 = keep * beta + step * alpha
    q2 = step * beta
    return 6.0 * q0, 6.0 * q1 - q0, 6.0 * q2 - q1, -q2


def kernel(
    counts, dims, chunks,
    res, den, base, yc, wout,
    held, dens, slots, comb, rhs, it, raw, pack, land, cland, yraw, ybuf, yland, xc,
    in_sem, den_sem, gsend, grecv, zsend, zrecv, ysend, yrecv, xsend, xrecv, csend, crecv,
):
    count, nz, ny, nx = dims
    cx, cy, cz = counts
    total_devices = cx * cy * cz
    h = SWEEPS
    ze = nz + 2 * h
    zp = yland.shape[1] // h
    tiles = ny // SUB
    ix, iy, iz = (lax.axis_index(a) for a in AXES)
    me = (ix * cy + iy) * cz + iz

    def near(dx, dy, dz):
        return (
            lax.rem(ix + dx + cx, cx),
            lax.rem(iy + dy + cy, cy),
            lax.rem(iz + dz + cz, cz),
        )

    barrier = pltpu.get_barrier_semaphore()

    offsets = [
        (dx, dy, dz) for dx in range(cx) for dy in range(cy) for dz in range(cz) if dx or dy or dz
    ]
    offsets.sort(key=lambda o: -sum(min(d, c - d) for d, c in zip(o, counts)))
    gx = [lax.rem(ix + d, cx) for d in range(cx)]
    gy = [lax.rem(iy + d, cy) for d in range(cy)]
    gz = [lax.rem(iz + d, cz) for d in range(cz)]
    for dx, dy, dz in offsets:
        pl.semaphore_signal(
            barrier, inc=1, device_id=(gx[dx], gy[dy], gz[dz]), device_id_type=MESH
        )

    per = nz // chunks
    loads = []
    for c in range(chunks):
        cp = pltpu.make_async_copy(
            res.at[:, pl.ds(c * per, per)], held.at[:, pl.ds(h + c * per, per)], in_sem.at[c]
        )
        cp.start()
        loads.append(cp)

    pairs = [(i, j) for i in range(count) for j in range(i, count)]
    accs = tuple(jnp.zeros((SUB, nx), jnp.float32) for _ in pairs)
    den_load = pltpu.make_async_copy(den, dens, den_sem)
    for c in range(chunks):
        loads[c].wait()
        if c == chunks - 1:
            den_load.start()

        def gram_step(z, accs):
            accs = list(accs)
            for t in range(tiles):
                v = [held[i, z, t * SUB:(t + 1) * SUB, :] for i in range(count)]
                for p, (i, j) in enumerate(pairs):
                    accs[p] = accs[p] + v[i] * v[j]
            return tuple(accs)

        accs = lax.fori_loop(h + c * per, h + (c + 1) * per, gram_step, accs)
    lane = lax.broadcasted_iota(jnp.int32, (SUB, nx), 1)
    packed = jnp.zeros((SUB, nx), jnp.float32)
    for p in range(len(pairs)):
        packed = jnp.where(lane == p, jnp.sum(accs[p], axis=1, keepdims=True), packed)
    slots[pl.ds(me, 1)] = jnp.sum(packed, axis=0, keepdims=True).reshape(1, 1, nx)

    pl.semaphore_wait(barrier, total_devices - 1)

    def gram_copy(k, slot):
        dx, dy, dz = offsets[k]
        return pltpu.make_async_remote_copy(
            src_ref=slots.at[me],
            dst_ref=slots.at[slot],
            send_sem=gsend.at[k],
            recv_sem=grecv.at[k],
            device_id=(gx[dx], gy[dy], gz[dz]),
            device_id_type=MESH,
        )

    for k in range(len(offsets)):
        gram_copy(k, me).start()

    zcopies = []
    for k, (start, dest, dz) in enumerate(((h, nz + h, -1), (nz, 0, 1))):
        cp = pltpu.make_async_remote_copy(
            src_ref=held.at[:, pl.ds(start, h)],
            dst_ref=held.at[:, pl.ds(dest, h)],
            send_sem=zsend.at[k],
            recv_sem=zrecv.at[k],
            device_id=near(0, 0, dz),
            device_id_type=MESH,
        )
        cp.start()
        zcopies.append(cp)

    def transfer(source, target, send_sem, recv_sem, dx, dy):
        cp = pltpu.make_async_remote_copy(
            src_ref=source,
            dst_ref=target,
            send_sem=send_sem,
            recv_sem=recv_sem,
            device_id=near(dx, dy, 0),
            device_id_type=MESH,
        )
        cp.start()
        return cp

    third = lane // h

    def gather_x(i, t, rows, head, tail):
        span = slice(t * SUB, (t + 1) * SUB)
        for z in rows:
            v = pltpu.roll(held[i, z, span, :], h * z + h, 1)
            head = jnp.where(third == z + 1, v, head)
            tail = jnp.where(third == z, v, tail)
        raw[i, 0, span, :] = head
        raw[i, 1, span, :] = tail

    def gather_y(i, rows):
        for z in rows:
            for k, t in enumerate((0, tiles - 1)):
                yraw[i, pl.ds(k * SUB * zp + (z - h) % zp, SUB, stride=zp), :] = held[
                    i, z, t * SUB:(t + 1) * SUB, :
                ]

    inner, outer = range(h, nz + h), (*range(h), *range(nz + h, ze))

    @pl.loop(0, count)
    def _(i):
        zero = jnp.zeros((SUB, nx), jnp.float32)
        for t in range(tiles):
            gather_x(i, t, inner, zero, zero)

    for cp in zcopies:
        cp.wait()
    for t in (0, tiles - 1, *range(1, tiles - 1)):
        span = slice(t * SUB, (t + 1) * SUB)
        for i in range(count):
            gather_x(i, t, outer, raw[i, 0, span, :], raw[i, 1, span, :])
    corners = []
    for k, dx in enumerate((-1, 1)):
        for end, (start, dy) in enumerate(((ny - SUB, 1), (0, -1))):
            corners.append(
                transfer(
                    raw.at[:, k, pl.ds(start, SUB)], cland.at[1 - k, end],
                    csend.at[k, end], crecv.at[k, end], dx, dy,
                )
            )

    @pl.loop(0, count)
    def _(i):
        gather_y(i, range(ze))

    for p in range(h, SUB):
        mirror = 2 * SUB - 1 - p
        yc[p * zp:(p + 1) * zp, :] = jnp.zeros((zp, nx), jnp.float32)
        yc[mirror * zp:(mirror + 1) * zp, :] = jnp.zeros((zp, nx), jnp.float32)

    for k, (dx, dy, dz) in enumerate(offsets):
        source = (gx[-dx % cx] * cy + gy[-dy % cy]) * cz + gz[-dz % cz]
        gram_copy(k, source).wait_recv()

    total = jnp.sum(slots[...], axis=0)

    g = {}
    for p, (i, j) in enumerate(pairs):
        g[i, j] = jnp.broadcast_to(total[:, p:p + 1], (SUB, nx))
    b = [jnp.ones((SUB, nx), jnp.float32) for _ in range(count)]
    inv = []
    for k in range(count):
        inv.append(1.0 / g[k, k])
        for i in range(k + 1, count):
            f = g[k, i] * inv[k]
            for j in range(i, count):
                g[i, j] = g[i, j] - f * g[k, j]
            b[i] = b[i] - f * b[k]
    solved = [None] * count
    for k in reversed(range(count)):
        solved[k] = b[k] * inv[k]
        for i in range(k):
            b[i] = b[i] - g[i, k] * solved[k]
    norm = solved[0]
    for k in range(1, count):
        norm = norm + solved[k]
    weights = [s / norm for s in solved]

    def blend(parts):
        s = weights[0] * parts(0)
        for i in range(1, count):
            s = s + weights[i] * parts(i)
        return s

    def combine_face(k):
        for p in range(h):
            source = (k * SUB + (p if k == 0 else SUB - 1 - p)) * zp
            for r in range(0, zp, SUB):
                ybuf[k, p * zp + r:p * zp + r + SUB, :] = blend(
                    lambda i: yraw[i, source + r:source + r + SUB, :]
                )

    def send_y(k, dy):
        message = pl.ds(0, h * zp - SUB)
        return transfer(
            ybuf.at[k, message], yland.at[1 - k, message], ysend.at[k], yrecv.at[k], 0, dy
        )

    combine_face(1)
    ycopies = [send_y(1, 1)]
    for k in range(2):
        for t in range(tiles):
            span = slice(t * SUB, (t + 1) * SUB)
            pack[k, span, :] = blend(lambda i: raw[i, k, span, :])
    combine_face(0)

    xcopies = [
        transfer(pack.at[k], land.at[1 - k, pl.ds(SUB, ny)], xsend.at[k], xrecv.at[k], dx, 0)
        for k, dx in enumerate((-1, 1))
    ]
    ycopies.append(send_y(0, -1))

    @pl.loop(0, ze // 2)
    def _(half):
        for r in range(2):
            z = half * 2 + r
            for t in range(tiles):
                span = slice(t * SUB, (t + 1) * SUB)
                comb[z, span, :] = blend(lambda i: held[i, z, span, :])

    row = jnp.zeros((SUB, nx), jnp.float32)
    for k in range(count):
        row = jnp.where(lane == k, weights[k], row)
    wout[...] = row[0:1, :count]

    def around(f, z):
        v = f[z]
        total = pltpu.roll(v, 1, 1) + pltpu.roll(v, nx - 1, 1)
        total = total + (pltpu.roll(v, 1, 0) + pltpu.roll(v, ny - 1, 0))
        return v, total + (f[z - 1] + f[z + 1])

    def planes(start, stop, unroll):
        steps = (stop - start) // unroll

        def wrap(body):
            @pl.loop(0, steps)
            def _(block):
                for r in range(unroll):
                    body(start + block * unroll + r)

            for z in range(start + steps * unroll, stop):
                body(z)
            return body

        return wrap

    alpha, beta, keep, step = sweep_factors()

    @planes(1, ze - 1, UNROLL)
    def _(z):
        v, total = around(comb, z)
        rhs[z] = 6.0 * v - total

    @planes(2, ze - 2, UNROLL)
    def _(z):
        v, total = around(rhs, z)
        it[z] = alpha * v + beta * total

    den_load.wait()

    @planes(h, nz + h, UNROLL)
    def _(z):
        v, total = around(it, z)
        u = keep * v + step * (rhs[z] + total)
        for t in range(tiles):
            span = slice(t * SUB, (t + 1) * SUB)
            base[z - h, span, :] = blend(lambda i: dens[i, z - h, span, :]) + u[span, :]

    _, c1, c2, c3 = neighbour_polynomial()

    def by_distance(first, second, square):
        near_by = (c1 + 3.0 * c3) * first + (2.0 * c2) * second + (3.0 * c3) * square
        return near_by, c2 * first + (3.0 * c3) * second

    wide = ny + 2 * SUB
    inside = slice(SUB, SUB + ny)
    column = lax.broadcasted_iota(jnp.int32, (ny, nx), 1)
    place = column % h

    def plane_sum(d):
        total = pltpu.roll(d, h, 1) + pltpu.roll(d, nx - h, 1)
        return total + (pltpu.roll(d, 1, 0) + pltpu.roll(d, wide - 1, 0))

    for cp in corners:
        cp.wait()
    for s in range(2):
        land[s, :SUB, :] = blend(lambda i: cland[s, 0, i])
        land[s, ny + SUB:, :] = blend(lambda i: cland[s, 1, i])
    for cp in xcopies:
        cp.wait()

    sides = []
    for s in range(2):
        own = pack[1 - s]
        d = land[s] - jnp.concatenate([own[ny - SUB:], own, own[:SUB]], axis=0)
        m = plane_sum(d)
        mm = plane_sum(m)
        a1, a2 = by_distance(d[inside], m[inside], mm[inside])
        a3 = c3 * d[inside]
        if s == 0:
            a1, a2, a3 = (pltpu.roll(a, k + 1, 1) for k, a in enumerate((a1, a2, a3)))
            depth = place
        else:
            a1, a2, a3 = (pltpu.roll(a, nx - k - 1, 1) for k, a in enumerate((a1, a2, a3)))
            depth = (h - 1) - place
        sides.append(
            jnp.where(depth == 0, a1, 0.0) + jnp.where(depth <= 1, a2, 0.0) + a3
        )
    even = (column // h) % 2 == 0
    xc[0] = jnp.where(even, sides[1], sides[0])
    xc[1] = jnp.where(even, sides[0], sides[1])

    edge = (lane < h) | (lane >= nx - h)
    for z in range(nz):
        e = z + h
        for t in range(tiles):
            span = slice(t * SUB, (t + 1) * SUB)
            v = pltpu.roll(xc[e % 2, span, :], (-(h * e + h)) % nx, 1)
            base[z, span, :] = base[z, span, :] + jnp.where(edge, v, 0.0)

    for cp in ycopies:
        cp.wait()

    along = lax.broadcasted_iota(jnp.int32, (zp, nx), 1)
    at_first, at_last = along == 0, along == nx - 1

    def face_sum(d):
        total = jnp.where(at_first, 0.0, pltpu.roll(d, 1, 1))
        total = total + jnp.where(at_last, 0.0, pltpu.roll(d, nx - 1, 1))
        return total + (pltpu.roll(d, 1, 0) + pltpu.roll(d, zp - 1, 0))

    for s in range(2):
        d1, d2 = (
            yland[s, k * zp:(k + 1) * zp, :] - ybuf[1 - s, k * zp:(k + 1) * zp, :]
            for k in range(2)
        )
        d3 = yland[s, 2 * zp:2 * zp + nz, :] - ybuf[1 - s, 2 * zp:2 * zp + nz, :]
        m = face_sum(d1)
        mm = face_sum(m) + jnp.where(at_first | at_last, d1, 0.0)
        near_1, near_2 = by_distance(d1[:nz], m[:nz], mm[:nz])
        rows = [
            near_1 + (c2 * d2 + (3.0 * c3) * face_sum(d2))[:nz] + c3 * d3,
            near_2 + c3 * d2[:nz],
            c3 * d1[:nz],
        ]
        for j, r in enumerate(rows):
            p = j if s == 0 else 2 * SUB - 1 - j
            yc[p * zp:p * zp + nz, :] = r

    for k in range(len(offsets)):
        gram_copy(k, me).wait_send()


def finish(base, yc, weights, out, wout, stage, sem, wsem):
    nz, ny, nx = base.shape
    zp = yc.shape[0] // (2 * SUB)
    pieces = sem.shape[0] - 1
    per = nz // pieces
    copies = []

    def store(source, target, sem):
        cp = pltpu.make_async_copy(source, target, sem)
        cp.start()
        copies.append(cp)

    store(weights, wout, wsem)
    if ny > 2 * SUB:
        middle = pl.ds(SUB, ny - 2 * SUB)
        store(base.at[:, middle], out.at[:, middle], sem.at[pieces, 0])
    for c in range(pieces):
        part = pl.ds(c * per, per)
        for k, start in enumerate((0, ny - SUB)):
            for z in range(c * per, (c + 1) * per):
                stage[k, z] = base[z, start:start + SUB, :] + yc[
                    pl.ds(k * SUB * zp + z, SUB, stride=zp), :
                ]
            store(stage.at[k, part], out.at[part, pl.ds(start, SUB)], sem.at[c, k])
    for cp in copies:
        cp.wait()


def on_device(counts, densities, residuals):
    dims = residuals.shape
    count, nz, ny, nx = dims
    h = SWEEPS
    ze = nz + 2 * h
    zp = pl.cdiv(ze, SUB) * SUB
    n = counts[0] * counts[1] * counts[2]
    chunks = 8
    tiles = ny // SUB
    assert tiles >= 2 and h * (ze + 1) <= nx
    dma = pltpu.SemaphoreType.DMA
    f32 = jnp.float32
    field = pltpu.VMEM((ze, ny, nx), f32)

    any_spec = pl.BlockSpec(memory_space=pl.ANY)
    vmem = pl.BlockSpec(memory_space=pltpu.VMEM)
    parts = pl.pallas_call(
        functools.partial(kernel, counts, dims, chunks),
        out_shape=(
            pltpu.VMEM((nz, ny, nx), f32),
            pltpu.VMEM((2 * SUB * zp, nx), f32),
            pltpu.VMEM((1, count), f32),
        ),
        in_specs=[any_spec, any_spec],
        out_specs=(vmem, vmem, vmem),
        scratch_shapes=[
            pltpu.VMEM((count, ze, ny, nx), f32),
            pltpu.VMEM(dims, f32),
            pltpu.VMEM((n, 1, nx), f32),
            field, field, field,
            pltpu.VMEM((count, 2, ny, nx), f32),
            pltpu.VMEM((2, ny, nx), f32),
            pltpu.VMEM((2, ny + 2 * SUB, nx), f32),
            pltpu.VMEM((2, 2, count, SUB, nx), f32),
            pltpu.VMEM((count, 2 * SUB * zp, nx), f32),
            pltpu.VMEM((2, h * zp, nx), f32),
            pltpu.VMEM((2, h * zp, nx), f32),
            pltpu.VMEM((2, ny, nx), f32),
            dma((chunks,)), dma(()), dma((n,)), dma((n,)),
            dma((2,)), dma((2,)), dma((2,)), dma((2,)), dma((2,)), dma((2,)), dma((2, 2)), dma((2, 2)),
        ],
        compiler_params=pltpu.CompilerParams(
            collective_id=0, has_side_effects=True, vmem_limit_bytes=56 * 1024 * 1024
        ),
    )(residuals, densities)
    new_density, weights = pl.pallas_call(
        finish,
        out_shape=(
            jax.ShapeDtypeStruct((nz, ny, nx), f32),
            jax.ShapeDtypeStruct((1, count), f32),
        ),
        in_specs=[vmem, vmem, vmem],
        out_specs=(any_spec, any_spec),
        scratch_shapes=[pltpu.VMEM((2, nz, SUB, nx), f32), dma((5, 2)), dma(())],
        compiler_params=pltpu.CompilerParams(vmem_limit_bytes=4 * 1024 * 1024),
    )(*parts)
    return new_density, weights.reshape(count)


def solution(mesh):
    counts = tuple(mesh.shape[a] for a in AXES)
    placed = (P(None, "gz", "gy", "gx"), P(None, "gz", "gy", "gx"))
    return jax.shard_map(
        functools.partial(on_device, counts),
        mesh=mesh,
        in_specs=placed,
        out_specs=(P("gz", "gy", "gx"), P()),
        check_vma=False,
    )
```

```python
import functools
import math

import jax
import jax.numpy as jnp
from jax import lax
from jax.experimental import pallas as pl
from jax.experimental.pallas import tpu as pltpu
from jax.sharding import PartitionSpec as P

MESH = pl.DeviceIdType.MESH
SWEEPS = 3
SUB = 8
UNROLL = 4
shift_value = 0.15
mix_amount = 0.7
AXES = ("gx", "gy", "gz")


def sweep_weights():
    diag_value = 6.0 + shift_value
    upper = (shift_value + 12.0) / diag_value
    lower = upper / 3.0
    return [
        1.0
        / (
            (upper + lower) / 2.0
            + (upper - lower) / 2.0 * math.cos(math.pi * (2 * k - 1) / (2 * SWEEPS))
        )
        for k in range(1, SWEEPS + 1)
    ]


def sweep_factors():
    diag_value = 6.0 + shift_value
    w1, w2, w3 = sweep_weights()
    alpha = ((1.0 - w2) * w1 + w2) / diag_value
    beta = w1 * w2 / (diag_value * diag_value)
    return alpha, beta, mix_amount * (1.0 - w3), mix_amount * w3 / diag_value


def neighbour_polynomial():
    alpha, beta, keep, step = sweep_factors()
    q0 = keep * alpha + step
    q1 = keep * beta + step * alpha
    q2 = step * beta
    return 6.0 * q0, 6.0 * q1 - q0, 6.0 * q2 - q1, -q2


def kernel(
    counts, dims, chunks,
    res, den, base, yc, wout,
    held, dens, slots, comb, rhs, it, raw, pack, land, cpack, cland, yraw, ybuf, yland, xc,
    in_sem, den_sem, gsend, grecv, zsend, zrecv, ysend, yrecv, xsend, xrecv, csend, crecv,
):
    count, nz, ny, nx = dims
    cx, cy, cz = counts
    total_devices = cx * cy * cz
    h = SWEEPS
    ze = nz + 2 * h
    zp = yland.shape[1] // h
    tiles = ny // SUB
    ix, iy, iz = (lax.axis_index(a) for a in AXES)
    me = (ix * cy + iy) * cz + iz

    def near(dx, dy, dz):
        return (
            lax.rem(ix + dx + cx, cx),
            lax.rem(iy + dy + cy, cy),
            lax.rem(iz + dz + cz, cz),
        )

    per = nz // chunks
    loads = []
    for c in range(chunks):
        cp = pltpu.make_async_copy(
            res.at[:, pl.ds(c * per, per)], held.at[:, pl.ds(h + c * per, per)], in_sem.at[c]
        )
        cp.start()
        loads.append(cp)

    barrier = pltpu.get_barrier_semaphore()

    offsets = [
        (dx, dy, dz) for dx in range(cx) for dy in range(cy) for dz in range(cz) if dx or dy or dz
    ]
    offsets.sort(key=lambda o: -sum(min(d, c - d) for d, c in zip(o, counts)))
    gx = [lax.rem(ix + d, cx) for d in range(cx)]
    gy = [lax.rem(iy + d, cy) for d in range(cy)]
    gz = [lax.rem(iz + d, cz) for d in range(cz)]
    for dx, dy, dz in offsets:
        pl.semaphore_signal(
            barrier, inc=1, device_id=(gx[dx], gy[dy], gz[dz]), device_id_type=MESH
        )

    pairs = [(i, j) for i in range(count) for j in range(i, count)]
    accs = tuple(jnp.zeros((SUB, nx), jnp.float32) for _ in pairs)
    den_load = pltpu.make_async_copy(den, dens, den_sem)
    for c in range(chunks):
        loads[c].wait()
        if c == chunks - 1:
            den_load.start()

        def gram_step(z, accs):
            accs = list(accs)
            for t in range(tiles):
                v = [held[i, z, t * SUB:(t + 1) * SUB, :] for i in range(count)]
                for p, (i, j) in enumerate(pairs):
                    accs[p] = accs[p] + v[i] * v[j]
            return tuple(accs)

        accs = lax.fori_loop(h + c * per, h + (c + 1) * per, gram_step, accs)
    lane = lax.broadcasted_iota(jnp.int32, (SUB, nx), 1)
    packed = jnp.zeros((SUB, nx), jnp.float32)
    for p in range(len(pairs)):
        packed = jnp.where(lane == p, jnp.sum(accs[p], axis=1, keepdims=True), packed)
    slots[pl.ds(me, 1)] = jnp.sum(packed, axis=0, keepdims=True).reshape(1, 1, nx)

    pl.semaphore_wait(barrier, total_devices - 1)

    def gram_copy(k, slot):
        dx, dy, dz = offsets[k]
        return pltpu.make_async_remote_copy(
            src_ref=slots.at[me],
            dst_ref=slots.at[slot],
            send_sem=gsend.at[k],
            recv_sem=grecv.at[k],
            device_id=(gx[dx], gy[dy], gz[dz]),
            device_id_type=MESH,
        )

    for k in range(len(offsets)):
        gram_copy(k, me).start()

    zcopies = []
    for k, (start, dest, dz) in enumerate(((h, nz + h, -1), (nz, 0, 1))):
        cp = pltpu.make_async_remote_copy(
            src_ref=held.at[:, pl.ds(start, h)],
            dst_ref=held.at[:, pl.ds(dest, h)],
            send_sem=zsend.at[k],
            recv_sem=zrecv.at[k],
            device_id=near(0, 0, dz),
            device_id_type=MESH,
        )
        cp.start()
        zcopies.append(cp)

    def transfer(source, target, send_sem, recv_sem, dx, dy):
        cp = pltpu.make_async_remote_copy(
            src_ref=source,
            dst_ref=target,
            send_sem=send_sem,
            recv_sem=recv_sem,
            device_id=near(dx, dy, 0),
            device_id_type=MESH,
        )
        cp.start()
        return cp

    third = lane // h

    def gather_x(i, t, rows, head, tail):
        span = slice(t * SUB, (t + 1) * SUB)
        for z in rows:
            v = pltpu.roll(held[i, z, span, :], h * z + h, 1)
            head = jnp.where(third == z + 1, v, head)
            tail = jnp.where(third == z, v, tail)
        raw[i, 0, span, :] = head
        raw[i, 1, span, :] = tail

    def gather_y(i, rows):
        for z in rows:
            for k, t in enumerate((0, tiles - 1)):
                yraw[i, pl.ds(k * SUB * zp + (z - h) % zp, SUB, stride=zp), :] = held[
                    i, z, t * SUB:(t + 1) * SUB, :
                ]

    inner, outer = range(h, nz + h), (*range(h), *range(nz + h, ze))

    @pl.loop(0, count)
    def _(i):
        zero = jnp.zeros((SUB, nx), jnp.float32)
        for t in range(tiles):
            gather_x(i, t, inner, zero, zero)

    for cp in zcopies:
        cp.wait()
    for t in (0, tiles - 1, *range(1, tiles - 1)):
        span = slice(t * SUB, (t + 1) * SUB)
        for i in range(count):
            gather_x(i, t, outer, raw[i, 0, span, :], raw[i, 1, span, :])

    corners = []
    flat_raw = raw.reshape(count * 2 * ny, nx)
    turn = (2, nx - 2)
    far = tuple(
        lax.broadcasted_iota(jnp.int32, (count, nx), 1) % h == c for c in (h - 1, 0)
    )
    for end, (first, second, dy) in enumerate(((ny - 1, ny - 2, 1), (0, 1, -1))):
        for k, dx in enumerate((-1, 1)):
            one, two = (
                flat_raw[pl.ds(k * ny + y, count, stride=2 * ny), :] for y in (first, second)
            )
            cpack[k, end] = jnp.where(far[k], pltpu.roll(two, turn[k], 1), one)
            corners.append(
                transfer(
                    cpack.at[k, end], cland.at[1 - k, end],
                    csend.at[k, end], crecv.at[k, end], dx, dy,
                )
            )

    @pl.loop(0, count)
    def _(i):
        gather_y(i, range(ze))

    for p in range(h, SUB):
        mirror = 2 * SUB - 1 - p
        yc[p * zp:(p + 1) * zp, :] = jnp.zeros((zp, nx), jnp.float32)
        yc[mirror * zp:(mirror + 1) * zp, :] = jnp.zeros((zp, nx), jnp.float32)

    for k, (dx, dy, dz) in enumerate(offsets):
        source = (gx[-dx % cx] * cy + gy[-dy % cy]) * cz + gz[-dz % cz]
        gram_copy(k, source).wait_recv()

    total = jnp.sum(slots[...], axis=0)

    g = {}
    for p, (i, j) in enumerate(pairs):
        g[i, j] = jnp.broadcast_to(total[:, p:p + 1], (SUB, nx))
    b = [jnp.ones((SUB, nx), jnp.float32) for _ in range(count)]
    inv = []
    for k in range(count):
        inv.append(1.0 / g[k, k])
        for i in range(k + 1, count):
            f = g[k, i] * inv[k]
            for j in range(i, count):
                g[i, j] = g[i, j] - f * g[k, j]
            b[i] = b[i] - f * b[k]
    solved = [None] * count
    for k in reversed(range(count)):
        solved[k] = b[k] * inv[k]
        for i in range(k):
            b[i] = b[i] - g[i, k] * solved[k]
    norm = solved[0]
    for k in range(1, count):
        norm = norm + solved[k]
    weights = [s / norm for s in solved]

    def blend(parts):
        s = weights[0] * parts(0)
        for i in range(1, count):
            s = s + weights[i] * parts(i)
        return s

    def combine_face(k):
        for p in range(h):
            source = (k * SUB + (p if k == 0 else SUB - 1 - p)) * zp
            for r in range(0, zp, SUB):
                ybuf[k, p * zp + r:p * zp + r + SUB, :] = blend(
                    lambda i: yraw[i, source + r:source + r + SUB, :]
                )

    def send_y(k, dy):
        message = pl.ds(0, h * zp - SUB)
        return transfer(
            ybuf.at[k, message], yland.at[1 - k, message], ysend.at[k], yrecv.at[k], 0, dy
        )

    combine_face(1)
    ycopies = [send_y(1, 1)]
    for k in range(2):
        for t in range(tiles):
            span = slice(t * SUB, (t + 1) * SUB)
            pack[k, span, :] = blend(lambda i: raw[i, k, span, :])
    combine_face(0)

    xcopies = [
        transfer(pack.at[k], land.at[1 - k, pl.ds(SUB, ny)], xsend.at[k], xrecv.at[k], dx, 0)
        for k, dx in enumerate((-1, 1))
    ]
    ycopies.append(send_y(0, -1))

    @pl.loop(0, ze // 2)
    def _(half):
        for r in range(2):
            z = half * 2 + r
            for t in range(tiles):
                span = slice(t * SUB, (t + 1) * SUB)
                comb[z, span, :] = blend(lambda i: held[i, z, span, :])

    row = jnp.zeros((SUB, nx), jnp.float32)
    for k in range(count):
        row = jnp.where(lane == k, weights[k], row)
    wout[...] = row[0:1, :count]

    def around(f, z):
        v = f[z]
        total = pltpu.roll(v, 1, 1) + pltpu.roll(v, nx - 1, 1)
        total = total + (pltpu.roll(v, 1, 0) + pltpu.roll(v, ny - 1, 0))
        return v, total + (f[z - 1] + f[z + 1])

    def planes(start, stop, unroll):
        steps = (stop - start) // unroll

        def wrap(body):
            @pl.loop(0, steps)
            def _(block):
                for r in range(unroll):
                    body(start + block * unroll + r)

            for z in range(start + steps * unroll, stop):
                body(z)
            return body

        return wrap

    alpha, beta, keep, step = sweep_factors()

    @planes(1, ze - 1, UNROLL)
    def _(z):
        v, total = around(comb, z)
        rhs[z] = 6.0 * v - total

    @planes(2, ze - 2, UNROLL)
    def _(z):
        v, total = around(rhs, z)
        it[z] = alpha * v + beta * total

    den_load.wait()

    @planes(h, nz + h, UNROLL)
    def _(z):
        v, total = around(it, z)
        u = keep * v + step * (rhs[z] + total)
        for t in range(tiles):
            span = slice(t * SUB, (t + 1) * SUB)
            base[z - h, span, :] = blend(lambda i: dens[i, z - h, span, :]) + u[span, :]

    _, c1, c2, c3 = neighbour_polynomial()

    def by_distance(first, second, square):
        near_by = (c1 + 3.0 * c3) * first + (2.0 * c2) * second + (3.0 * c3) * square
        return near_by, c2 * first + (3.0 * c3) * second

    wide = ny + 2 * SUB
    inside = slice(SUB, SUB + ny)
    column = lax.broadcasted_iota(jnp.int32, (ny, nx), 1)
    place = column % h

    def plane_sum(d):
        total = pltpu.roll(d, h, 1) + pltpu.roll(d, nx - h, 1)
        return total + (pltpu.roll(d, 1, 0) + pltpu.roll(d, wide - 1, 0))

    for cp in corners:
        cp.wait()
    sub = lax.broadcasted_iota(jnp.int32, (SUB, nx), 0)
    for s in range(2):
        for end, (start, nearest) in enumerate(((0, SUB - 1), (ny + SUB, 0))):
            found = blend(lambda i: jnp.broadcast_to(cland[s, end, i:i + 1, :], (SUB, nx)))
            land[s, start:start + SUB, :] = jnp.where(
                sub == nearest, found, pltpu.roll(found, turn[s], 1)
            )
    for cp in xcopies:
        cp.wait()

    sides = []
    for s in range(2):
        own = pack[1 - s]
        d = land[s] - jnp.concatenate([own[ny - SUB:], own, own[:SUB]], axis=0)
        m = plane_sum(d)
        mm = plane_sum(m)
        a1, a2 = by_distance(d[inside], m[inside], mm[inside])
        a3 = c3 * d[inside]
        if s == 0:
            a1, a2, a3 = (pltpu.roll(a, k + 1, 1) for k, a in enumerate((a1, a2, a3)))
            depth = place
        else:
            a1, a2, a3 = (pltpu.roll(a, nx - k - 1, 1) for k, a in enumerate((a1, a2, a3)))
            depth = (h - 1) - place
        sides.append(
            jnp.where(depth == 0, a1, 0.0) + jnp.where(depth <= 1, a2, 0.0) + a3
        )
    even = (column // h) % 2 == 0
    xc[0] = jnp.where(even, sides[1], sides[0])
    xc[1] = jnp.where(even, sides[0], sides[1])

    edge = (lane < h) | (lane >= nx - h)
    for z in range(nz):
        e = z + h
        for t in range(tiles):
            span = slice(t * SUB, (t + 1) * SUB)
            v = pltpu.roll(xc[e % 2, span, :], (-(h * e + h)) % nx, 1)
            base[z, span, :] = base[z, span, :] + jnp.where(edge, v, 0.0)

    for cp in ycopies:
        cp.wait()

    along = lax.broadcasted_iota(jnp.int32, (zp, nx), 1)
    at_first, at_last = along == 0, along == nx - 1

    def face_sum(d):
        total = jnp.where(at_first, 0.0, pltpu.roll(d, 1, 1))
        total = total + jnp.where(at_last, 0.0, pltpu.roll(d, nx - 1, 1))
        return total + (pltpu.roll(d, 1, 0) + pltpu.roll(d, zp - 1, 0))

    for s in range(2):
        d1, d2 = (
            yland[s, k * zp:(k + 1) * zp, :] - ybuf[1 - s, k * zp:(k + 1) * zp, :]
            for k in range(2)
        )
        d3 = yland[s, 2 * zp:2 * zp + nz, :] - ybuf[1 - s, 2 * zp:2 * zp + nz, :]
        m = face_sum(d1)
        mm = face_sum(m) + jnp.where(at_first | at_last, d1, 0.0)
        near_1, near_2 = by_distance(d1[:nz], m[:nz], mm[:nz])
        rows = [
            near_1 + (c2 * d2 + (3.0 * c3) * face_sum(d2))[:nz] + c3 * d3,
            near_2 + c3 * d2[:nz],
            c3 * d1[:nz],
        ]
        for j, r in enumerate(rows):
            p = j if s == 0 else 2 * SUB - 1 - j
            yc[p * zp:p * zp + nz, :] = r

    for k in range(len(offsets)):
        gram_copy(k, me).wait_send()


def finish(base, yc, weights, out, wout, stage, sem, wsem):
    nz, ny, nx = base.shape
    zp = yc.shape[0] // (2 * SUB)
    pieces = sem.shape[0] - 1
    per = nz // pieces
    copies = []

    def store(source, target, sem):
        cp = pltpu.make_async_copy(source, target, sem)
        cp.start()
        copies.append(cp)

    store(weights, wout, wsem)
    if ny > 2 * SUB:
        middle = pl.ds(SUB, ny - 2 * SUB)
        store(base.at[:, middle], out.at[:, middle], sem.at[pieces, 0])
    for c in range(pieces):
        part = pl.ds(c * per, per)
        for k, start in enumerate((0, ny - SUB)):
            for z in range(c * per, (c + 1) * per):
                stage[k, z] = base[z, start:start + SUB, :] + yc[
                    pl.ds(k * SUB * zp + z, SUB, stride=zp), :
                ]
            store(stage.at[k, part], out.at[part, pl.ds(start, SUB)], sem.at[c, k])
    for cp in copies:
        cp.wait()


def on_device(counts, densities, residuals):
    dims = residuals.shape
    count, nz, ny, nx = dims
    h = SWEEPS
    ze = nz + 2 * h
    zp = pl.cdiv(ze, SUB) * SUB
    n = counts[0] * counts[1] * counts[2]
    chunks = 8
    tiles = ny // SUB
    assert tiles >= 2 and h * (ze + 1) <= nx
    dma = pltpu.SemaphoreType.DMA
    f32 = jnp.float32
    field = pltpu.VMEM((ze, ny, nx), f32)

    any_spec = pl.BlockSpec(memory_space=pl.ANY)
    vmem = pl.BlockSpec(memory_space=pltpu.VMEM)
    parts = pl.pallas_call(
        functools.partial(kernel, counts, dims, chunks),
        out_shape=(
            pltpu.VMEM((nz, ny, nx), f32),
            pltpu.VMEM((2 * SUB * zp, nx), f32),
            pltpu.VMEM((1, count), f32),
        ),
        in_specs=[any_spec, any_spec],
        out_specs=(vmem, vmem, vmem),
        scratch_shapes=[
            pltpu.VMEM((count, ze, ny, nx), f32),
            pltpu.VMEM(dims, f32),
            pltpu.VMEM((n, 1, nx), f32),
            field, field, field,
            pltpu.VMEM((count, 2, ny, nx), f32),
            pltpu.VMEM((2, ny, nx), f32),
            pltpu.VMEM((2, ny + 2 * SUB, nx), f32),
            pltpu.VMEM((2, 2, count, nx), f32),
            pltpu.VMEM((2, 2, count, nx), f32),
            pltpu.VMEM((count, 2 * SUB * zp, nx), f32),
            pltpu.VMEM((2, h * zp, nx), f32),
            pltpu.VMEM((2, h * zp, nx), f32),
            pltpu.VMEM((2, ny, nx), f32),
            dma((chunks,)), dma(()), dma((n,)), dma((n,)),
            dma((2,)), dma((2,)), dma((2,)), dma((2,)), dma((2,)), dma((2,)), dma((2, 2)), dma((2, 2)),
        ],
        compiler_params=pltpu.CompilerParams(
            collective_id=0, has_side_effects=True, vmem_limit_bytes=56 * 1024 * 1024
        ),
    )(residuals, densities)
    new_density, weights = pl.pallas_call(
        finish,
        out_shape=(
            jax.ShapeDtypeStruct((nz, ny, nx), f32),
            jax.ShapeDtypeStruct((1, count), f32),
        ),
        in_specs=[vmem, vmem, vmem],
        out_specs=(any_spec, any_spec),
        scratch_shapes=[pltpu.VMEM((2, nz, SUB, nx), f32), dma((5, 2)), dma(())],
        compiler_params=pltpu.CompilerParams(vmem_limit_bytes=4 * 1024 * 1024),
    )(*parts)
    return new_density, weights.reshape(count)


def solution(mesh):
    counts = tuple(mesh.shape[a] for a in AXES)
    placed = (P(None, "gz", "gy", "gx"), P(None, "gz", "gy", "gx"))
    return jax.shard_map(
        functools.partial(on_device, counts),
        mesh=mesh,
        in_specs=placed,
        out_specs=(P("gz", "gy", "gx"), P()),
        check_vma=False,
    )
```

```python
import functools
import math

import jax
import jax.numpy as jnp
from jax import lax
from jax.experimental import pallas as pl
from jax.experimental.pallas import tpu as pltpu
from jax.sharding import PartitionSpec as P

MESH = pl.DeviceIdType.MESH
SWEEPS = 3
SUB = 8
UNROLL = 12
shift_value = 0.15
mix_amount = 0.7
AXES = ("gx", "gy", "gz")


def sweep_weights():
    diag_value = 6.0 + shift_value
    upper = (shift_value + 12.0) / diag_value
    lower = upper / 3.0
    return [
        1.0
        / (
            (upper + lower) / 2.0
            + (upper - lower) / 2.0 * math.cos(math.pi * (2 * k - 1) / (2 * SWEEPS))
        )
        for k in range(1, SWEEPS + 1)
    ]


def sweep_factors():
    diag_value = 6.0 + shift_value
    w1, w2, w3 = sweep_weights()
    alpha = ((1.0 - w2) * w1 + w2) / diag_value
    beta = w1 * w2 / (diag_value * diag_value)
    return alpha, beta, mix_amount * (1.0 - w3), mix_amount * w3 / diag_value


def neighbour_polynomial():
    alpha, beta, keep, step = sweep_factors()
    q0 = keep * alpha + step
    q1 = keep * beta + step * alpha
    q2 = step * beta
    return 6.0 * q0, 6.0 * q1 - q0, 6.0 * q2 - q1, -q2


def kernel(
    counts, dims, chunks,
    res, den, base, yc, wout,
    held, dens, slots, comb, rhs, it, raw, pack, land, cpack, cland, yraw, ybuf, yland, xc,
    in_sem, den_sem, gsend, grecv, zsend, zrecv, ysend, yrecv, xsend, xrecv, csend, crecv,
):
    count, nz, ny, nx = dims
    cx, cy, cz = counts
    total_devices = cx * cy * cz
    h = SWEEPS
    ze = nz + 2 * h
    zp = yland.shape[1] // h
    tiles = ny // SUB
    ix, iy, iz = (lax.axis_index(a) for a in AXES)
    me = (ix * cy + iy) * cz + iz

    def near(dx, dy, dz):
        return (
            lax.rem(ix + dx + cx, cx),
            lax.rem(iy + dy + cy, cy),
            lax.rem(iz + dz + cz, cz),
        )

    per = nz // chunks
    loads = []
    for c in range(chunks):
        cp = pltpu.make_async_copy(
            res.at[:, pl.ds(c * per, per)], held.at[:, pl.ds(h + c * per, per)], in_sem.at[c]
        )
        cp.start()
        loads.append(cp)

    barrier = pltpu.get_barrier_semaphore()

    offsets = [
        (dx, dy, dz) for dx in range(cx) for dy in range(cy) for dz in range(cz) if dx or dy or dz
    ]
    offsets.sort(key=lambda o: -sum(min(d, c - d) for d, c in zip(o, counts)))
    gx = [lax.rem(ix + d, cx) for d in range(cx)]
    gy = [lax.rem(iy + d, cy) for d in range(cy)]
    gz = [lax.rem(iz + d, cz) for d in range(cz)]
    for dx, dy, dz in offsets:
        pl.semaphore_signal(
            barrier, inc=1, device_id=(gx[dx], gy[dy], gz[dz]), device_id_type=MESH
        )

    pairs = [(i, j) for i in range(count) for j in range(i, count)]
    accs = tuple(jnp.zeros((SUB, nx), jnp.float32) for _ in pairs)
    den_load = pltpu.make_async_copy(den, dens, den_sem)
    for c in range(chunks):
        loads[c].wait()
        if c == chunks - 1:
            den_load.start()

        def gram_step(z, accs):
            accs = list(accs)
            for t in range(tiles):
                v = [held[i, z, t * SUB:(t + 1) * SUB, :] for i in range(count)]
                for p, (i, j) in enumerate(pairs):
                    accs[p] = accs[p] + v[i] * v[j]
            return tuple(accs)

        accs = lax.fori_loop(h + c * per, h + (c + 1) * per, gram_step, accs)
    lane = lax.broadcasted_iota(jnp.int32, (SUB, nx), 1)
    packed = jnp.zeros((SUB, nx), jnp.float32)
    for p in range(len(pairs)):
        packed = jnp.where(lane == p, jnp.sum(accs[p], axis=1, keepdims=True), packed)
    slots[pl.ds(me, 1)] = jnp.sum(packed, axis=0, keepdims=True).reshape(1, 1, nx)

    pl.semaphore_wait(barrier, total_devices - 1)

    def gram_copy(k):
        dx, dy, dz = offsets[k]
        return pltpu.make_async_remote_copy(
            src_ref=slots.at[me],
            dst_ref=slots.at[me],
            send_sem=gsend,
            recv_sem=grecv,
            device_id=(gx[dx], gy[dy], gz[dz]),
            device_id_type=MESH,
        )

    for k in range(len(offsets)):
        gram_copy(k).start()

    def all_of(ref, send_sem, recv_sem):
        return pltpu.make_async_remote_copy(
            src_ref=ref,
            dst_ref=ref,
            send_sem=send_sem,
            recv_sem=recv_sem,
            device_id=near(0, 0, 1),
            device_id_type=MESH,
        )

    for k, (start, dest, dz) in enumerate(((h, nz + h, -1), (nz, 0, 1))):
        cp = pltpu.make_async_remote_copy(
            src_ref=held.at[:, pl.ds(start, h)],
            dst_ref=held.at[:, pl.ds(dest, h)],
            send_sem=zsend,
            recv_sem=zrecv,
            device_id=near(0, 0, dz),
            device_id_type=MESH,
        )
        cp.start()

    def transfer(source, target, send_sem, recv_sem, dx, dy):
        cp = pltpu.make_async_remote_copy(
            src_ref=source,
            dst_ref=target,
            send_sem=send_sem,
            recv_sem=recv_sem,
            device_id=near(dx, dy, 0),
            device_id_type=MESH,
        )
        cp.start()

    third = lane // h

    def gather_x(i, t, rows, head, tail):
        span = slice(t * SUB, (t + 1) * SUB)
        for z in rows:
            v = pltpu.roll(held[i, z, span, :], h * z + h, 1)
            head = jnp.where(third == z + 1, v, head)
            tail = jnp.where(third == z, v, tail)
        raw[i, 0, span, :] = head
        raw[i, 1, span, :] = tail

    def gather_y(i, rows):
        for z in rows:
            for k, t in enumerate((0, tiles - 1)):
                yraw[i, pl.ds(k * SUB * zp + (z - h) % zp, SUB, stride=zp), :] = held[
                    i, z, t * SUB:(t + 1) * SUB, :
                ]

    inner, outer = range(h, nz + h), (*range(h), *range(nz + h, ze))

    @pl.loop(0, count)
    def _(i):
        zero = jnp.zeros((SUB, nx), jnp.float32)
        for t in range(tiles):
            gather_x(i, t, inner, zero, zero)

    all_of(held.at[:, pl.ds(0, 2 * h)], zsend, zrecv).wait()
    for t in (0, tiles - 1, *range(1, tiles - 1)):
        span = slice(t * SUB, (t + 1) * SUB)
        for i in range(count):
            gather_x(i, t, outer, raw[i, 0, span, :], raw[i, 1, span, :])

    flat_raw = raw.reshape(count * 2 * ny, nx)
    turn = (2, nx - 2)
    far = tuple(
        lax.broadcasted_iota(jnp.int32, (count, nx), 1) % h == c for c in (h - 1, 0)
    )
    for end, (first, second, dy) in enumerate(((ny - 1, ny - 2, 1), (0, 1, -1))):
        for k, dx in enumerate((-1, 1)):
            one, two = (
                flat_raw[pl.ds(k * ny + y, count, stride=2 * ny), :] for y in (first, second)
            )
            cpack[k, end] = jnp.where(far[k], pltpu.roll(two, turn[k], 1), one)
            transfer(cpack.at[k, end], cland.at[1 - k, end], csend, crecv, dx, dy)

    @pl.loop(0, count)
    def _(i):
        gather_y(i, range(ze))

    for p in range(h, SUB):
        mirror = 2 * SUB - 1 - p
        yc[p * zp:(p + 1) * zp, :] = jnp.zeros((zp, nx), jnp.float32)
        yc[mirror * zp:(mirror + 1) * zp, :] = jnp.zeros((zp, nx), jnp.float32)

    gram_all = all_of(slots.at[pl.ds(0, total_devices - 1)], gsend, grecv)
    gram_all.wait_recv()

    total = jnp.sum(slots[...], axis=0)

    g = {}
    for p, (i, j) in enumerate(pairs):
        g[i, j] = jnp.broadcast_to(total[:, p:p + 1], (SUB, nx))
    b = [jnp.ones((SUB, nx), jnp.float32) for _ in range(count)]
    inv = []
    for k in range(count):
        inv.append(1.0 / g[k, k])
        for i in range(k + 1, count):
            f = g[k, i] * inv[k]
            for j in range(i, count):
                g[i, j] = g[i, j] - f * g[k, j]
            b[i] = b[i] - f * b[k]
    solved = [None] * count
    for k in reversed(range(count)):
        solved[k] = b[k] * inv[k]
        for i in range(k):
            b[i] = b[i] - g[i, k] * solved[k]
    norm = solved[0]
    for k in range(1, count):
        norm = norm + solved[k]
    weights = [s / norm for s in solved]

    def blend(parts):
        s = weights[0] * parts(0)
        for i in range(1, count):
            s = s + weights[i] * parts(i)
        return s

    def combine_face(k):
        for p in range(h):
            source = (k * SUB + (p if k == 0 else SUB - 1 - p)) * zp
            for r in range(0, zp, SUB):
                ybuf[k, p * zp + r:p * zp + r + SUB, :] = blend(
                    lambda i: yraw[i, source + r:source + r + SUB, :]
                )

    message = pl.ds(0, h * zp - SUB)

    def send_y(k, dy):
        transfer(ybuf.at[k, message], yland.at[1 - k, message], ysend, yrecv, 0, dy)

    combine_face(1)
    send_y(1, 1)
    for k in range(2):
        for t in range(tiles):
            span = slice(t * SUB, (t + 1) * SUB)
            pack[k, span, :] = blend(lambda i: raw[i, k, span, :])
    combine_face(0)

    for k, dx in enumerate((-1, 1)):
        transfer(pack.at[k], land.at[1 - k, pl.ds(SUB, ny)], xsend, xrecv, dx, 0)
    send_y(0, -1)

    @pl.loop(0, ze // 2)
    def _(half):
        for r in range(2):
            z = half * 2 + r
            for t in range(tiles):
                span = slice(t * SUB, (t + 1) * SUB)
                comb[z, span, :] = blend(lambda i: held[i, z, span, :])

    row = jnp.zeros((SUB, nx), jnp.float32)
    for k in range(count):
        row = jnp.where(lane == k, weights[k], row)
    wout[...] = row[0:1, :count]

    def around(f, z):
        v = f[z]
        total = pltpu.roll(v, 1, 1) + pltpu.roll(v, nx - 1, 1)
        total = total + (pltpu.roll(v, 1, 0) + pltpu.roll(v, ny - 1, 0))
        return v, total + (f[z - 1] + f[z + 1])

    def planes(start, stop, unroll):
        steps = (stop - start) // unroll

        def wrap(body):
            @pl.loop(0, steps)
            def _(block):
                for r in range(unroll):
                    body(start + block * unroll + r)

            for z in range(start + steps * unroll, stop):
                body(z)
            return body

        return wrap

    alpha, beta, keep, step = sweep_factors()

    @planes(1, ze - 1, UNROLL)
    def _(z):
        v, total = around(comb, z)
        rhs[z] = 6.0 * v - total

    @planes(2, ze - 2, UNROLL)
    def _(z):
        v, total = around(rhs, z)
        it[z] = alpha * v + beta * total

    den_load.wait()

    @planes(h, nz + h, UNROLL)
    def _(z):
        v, total = around(it, z)
        u = keep * v + step * (rhs[z] + total)
        for t in range(tiles):
            span = slice(t * SUB, (t + 1) * SUB)
            base[z - h, span, :] = blend(lambda i: dens[i, z - h, span, :]) + u[span, :]

    _, c1, c2, c3 = neighbour_polynomial()

    def by_distance(first, second, square):
        near_by = (c1 + 3.0 * c3) * first + (2.0 * c2) * second + (3.0 * c3) * square
        return near_by, c2 * first + (3.0 * c3) * second

    wide = ny + 2 * SUB
    inside = slice(SUB, SUB + ny)
    column = lax.broadcasted_iota(jnp.int32, (ny, nx), 1)
    place = column % h

    def plane_sum(d):
        total = pltpu.roll(d, h, 1) + pltpu.roll(d, nx - h, 1)
        return total + (pltpu.roll(d, 1, 0) + pltpu.roll(d, wide - 1, 0))

    all_of(cland, csend, crecv).wait()
    sub = lax.broadcasted_iota(jnp.int32, (SUB, nx), 0)
    for s in range(2):
        for end, (start, nearest) in enumerate(((0, SUB - 1), (ny + SUB, 0))):
            found = blend(lambda i: jnp.broadcast_to(cland[s, end, i:i + 1, :], (SUB, nx)))
            land[s, start:start + SUB, :] = jnp.where(
                sub == nearest, found, pltpu.roll(found, turn[s], 1)
            )
    all_of(land.at[:, pl.ds(SUB, ny)], xsend, xrecv).wait()

    sides = []
    for s in range(2):
        own = pack[1 - s]
        d = land[s] - jnp.concatenate([own[ny - SUB:], own, own[:SUB]], axis=0)
        m = plane_sum(d)
        mm = plane_sum(m)
        a1, a2 = by_distance(d[inside], m[inside], mm[inside])
        a3 = c3 * d[inside]
        if s == 0:
            a1, a2, a3 = (pltpu.roll(a, k + 1, 1) for k, a in enumerate((a1, a2, a3)))
            depth = place
        else:
            a1, a2, a3 = (pltpu.roll(a, nx - k - 1, 1) for k, a in enumerate((a1, a2, a3)))
            depth = (h - 1) - place
        sides.append(
            jnp.where(depth == 0, a1, 0.0) + jnp.where(depth <= 1, a2, 0.0) + a3
        )
    even = (column // h) % 2 == 0
    xc[0] = jnp.where(even, sides[1], sides[0])
    xc[1] = jnp.where(even, sides[0], sides[1])

    edge = (lane < h) | (lane >= nx - h)
    for z in range(nz):
        e = z + h
        for t in range(tiles):
            span = slice(t * SUB, (t + 1) * SUB)
            v = pltpu.roll(xc[e % 2, span, :], (-(h * e + h)) % nx, 1)
            base[z, span, :] = base[z, span, :] + jnp.where(edge, v, 0.0)

    all_of(yland.at[:, message], ysend, yrecv).wait()

    along = lax.broadcasted_iota(jnp.int32, (zp, nx), 1)
    at_first, at_last = along == 0, along == nx - 1

    def face_sum(d):
        total = jnp.where(at_first, 0.0, pltpu.roll(d, 1, 1))
        total = total + jnp.where(at_last, 0.0, pltpu.roll(d, nx - 1, 1))
        return total + (pltpu.roll(d, 1, 0) + pltpu.roll(d, zp - 1, 0))

    for s in range(2):
        d1, d2 = (
            yland[s, k * zp:(k + 1) * zp, :] - ybuf[1 - s, k * zp:(k + 1) * zp, :]
            for k in range(2)
        )
        d3 = yland[s, 2 * zp:2 * zp + nz, :] - ybuf[1 - s, 2 * zp:2 * zp + nz, :]
        m = face_sum(d1)
        mm = face_sum(m) + jnp.where(at_first | at_last, d1, 0.0)
        near_1, near_2 = by_distance(d1[:nz], m[:nz], mm[:nz])
        rows = [
            near_1 + (c2 * d2 + (3.0 * c3) * face_sum(d2))[:nz] + c3 * d3,
            near_2 + c3 * d2[:nz],
            c3 * d1[:nz],
        ]
        for j, r in enumerate(rows):
            p = j if s == 0 else 2 * SUB - 1 - j
            yc[p * zp:p * zp + nz, :] = r

    gram_all.wait_send()


def finish(base, yc, weights, out, wout, stage, sem, wsem):
    nz, ny, nx = base.shape
    zp = yc.shape[0] // (2 * SUB)
    pieces = 4
    per = nz // pieces

    def store(source, target):
        pltpu.make_async_copy(source, target, sem).start()

    wcopy = pltpu.make_async_copy(weights, wout, wsem)
    wcopy.start()
    if ny > 2 * SUB:
        middle = pl.ds(SUB, ny - 2 * SUB)
        store(base.at[:, middle], out.at[:, middle])
    for c in range(pieces):
        part = pl.ds(c * per, per)
        for k, start in enumerate((0, ny - SUB)):
            for z in range(c * per, (c + 1) * per):
                stage[k, z] = base[z, start:start + SUB, :] + yc[
                    pl.ds(k * SUB * zp + z, SUB, stride=zp), :
                ]
            store(stage.at[k, part], out.at[part, pl.ds(start, SUB)])
    pltpu.make_async_copy(base, out, sem).wait()
    wcopy.wait()


def on_device(counts, densities, residuals):
    dims = residuals.shape
    count, nz, ny, nx = dims
    h = SWEEPS
    ze = nz + 2 * h
    zp = pl.cdiv(ze, SUB) * SUB
    n = counts[0] * counts[1] * counts[2]
    chunks = 8
    tiles = ny // SUB
    assert tiles >= 2 and h * (ze + 1) <= nx
    dma = pltpu.SemaphoreType.DMA
    f32 = jnp.float32
    field = pltpu.VMEM((ze, ny, nx), f32)

    any_spec = pl.BlockSpec(memory_space=pl.ANY)
    vmem = pl.BlockSpec(memory_space=pltpu.VMEM)
    parts = pl.pallas_call(
        functools.partial(kernel, counts, dims, chunks),
        out_shape=(
            pltpu.VMEM((nz, ny, nx), f32),
            pltpu.VMEM((2 * SUB * zp, nx), f32),
            pltpu.VMEM((1, count), f32),
        ),
        in_specs=[any_spec, any_spec],
        out_specs=(vmem, vmem, vmem),
        scratch_shapes=[
            pltpu.VMEM((count, ze, ny, nx), f32),
            pltpu.VMEM(dims, f32),
            pltpu.VMEM((n, 1, nx), f32),
            field, field, field,
            pltpu.VMEM((count, 2, ny, nx), f32),
            pltpu.VMEM((2, ny, nx), f32),
            pltpu.VMEM((2, ny + 2 * SUB, nx), f32),
            pltpu.VMEM((2, 2, count, nx), f32),
            pltpu.VMEM((2, 2, count, nx), f32),
            pltpu.VMEM((count, 2 * SUB * zp, nx), f32),
            pltpu.VMEM((2, h * zp, nx), f32),
            pltpu.VMEM((2, h * zp, nx), f32),
            pltpu.VMEM((2, ny, nx), f32),
            dma((chunks,)), *(dma(()) for _ in range(11)),
        ],
        compiler_params=pltpu.CompilerParams(
            collective_id=0, has_side_effects=True, vmem_limit_bytes=56 * 1024 * 1024
        ),
    )(residuals, densities)
    new_density, weights = pl.pallas_call(
        finish,
        out_shape=(
            jax.ShapeDtypeStruct((nz, ny, nx), f32),
            jax.ShapeDtypeStruct((1, count), f32),
        ),
        in_specs=[vmem, vmem, vmem],
        out_specs=(any_spec, any_spec),
        scratch_shapes=[pltpu.VMEM((2, nz, SUB, nx), f32), dma(()), dma(())],
        compiler_params=pltpu.CompilerParams(vmem_limit_bytes=4 * 1024 * 1024),
    )(*parts)
    return new_density, weights.reshape(count)


def solution(mesh):
    counts = tuple(mesh.shape[a] for a in AXES)
    placed = (P(None, "gz", "gy", "gx"), P(None, "gz", "gy", "gx"))
    return jax.shard_map(
        functools.partial(on_device, counts),
        mesh=mesh,
        in_specs=placed,
        out_specs=(P("gz", "gy", "gx"), P()),
        check_vma=False,
    )
```

```python
import functools
import math

import jax
import jax.numpy as jnp
from jax import lax
from jax.experimental import pallas as pl
from jax.experimental.pallas import tpu as pltpu
from jax.sharding import PartitionSpec as P

MESH = pl.DeviceIdType.MESH
SWEEPS = 3
SUB = 8
UNROLL = 12
shift_value = 0.15
mix_amount = 0.7
AXES = ("gx", "gy", "gz")


def sweep_weights():
    diag_value = 6.0 + shift_value
    upper = (shift_value + 12.0) / diag_value
    lower = upper / 3.0
    return [
        1.0
        / (
            (upper + lower) / 2.0
            + (upper - lower) / 2.0 * math.cos(math.pi * (2 * k - 1) / (2 * SWEEPS))
        )
        for k in range(1, SWEEPS + 1)
    ]


def sweep_factors():
    diag_value = 6.0 + shift_value
    w1, w2, w3 = sweep_weights()
    alpha = ((1.0 - w2) * w1 + w2) / diag_value
    beta = w1 * w2 / (diag_value * diag_value)
    return alpha, beta, mix_amount * (1.0 - w3), mix_amount * w3 / diag_value


def neighbour_polynomial():
    alpha, beta, keep, step = sweep_factors()
    q0 = keep * alpha + step
    q1 = keep * beta + step * alpha
    q2 = step * beta
    return 6.0 * q0, 6.0 * q1 - q0, 6.0 * q2 - q1, -q2


def kernel(
    counts, dims, chunks,
    res, den, base, yc, wout,
    held, dens, slots, comb, rhs, it, raw, pack, land, cpack, cland,
    yraw, ycon, ymate, ymix, ybuf, yland, xc,
    in_sem, den_sem, sent, grecv, zrecv, mrecv, xrecv, yrecv,
):
    count, nz, ny, nx = dims
    cx, cy, cz = counts
    total_devices = cx * cy * cz
    h = SWEEPS
    ze = nz + 2 * h
    zp = yraw.shape[1] // (2 * SUB)
    tiles = ny // SUB
    ix, iy, iz = (lax.axis_index(a) for a in AXES)
    me = (ix * cy + iy) * cz + iz

    def near(dx, dy, dz):
        return (
            lax.rem(ix + dx + cx, cx),
            lax.rem(iy + dy + cy, cy),
            lax.rem(iz + dz + cz, cz),
        )

    loads, first = [], 0
    for c, size in enumerate(chunks):
        cp = pltpu.make_async_copy(
            res.at[:, pl.ds(first, size)], held.at[:, pl.ds(h + first, size)], in_sem.at[c]
        )
        cp.start()
        loads.append((cp, h + first, h + first + size))
        first += size

    barrier = pltpu.get_barrier_semaphore()

    offsets = [
        (dx, dy, dz) for dx in range(cx) for dy in range(cy) for dz in range(cz) if dx or dy or dz
    ]
    order = [1, cy - 1, *range(2, cy - 1), 0]
    offsets.sort(key=lambda o: (-(o[0] % 2), order.index(o[1])))
    gx = [lax.rem(ix + d, cx) for d in range(cx)]
    gy = [lax.rem(iy + d, cy) for d in range(cy)]
    gz = [lax.rem(iz + d, cz) for d in range(cz)]
    for dx, dy, dz in offsets:
        pl.semaphore_signal(
            barrier, inc=1, device_id=(gx[dx], gy[dy], gz[dz]), device_id_type=MESH
        )

    pairs = [(i, j) for i in range(count) for j in range(i, count)]
    accs = tuple(jnp.zeros((SUB, nx), jnp.float32) for _ in pairs)
    den_load = pltpu.make_async_copy(den, dens, den_sem)
    for c, (load, start, stop) in enumerate(loads):
        load.wait()
        if c == len(loads) - 1:
            den_load.start()

        def gram_step(z, accs):
            accs = list(accs)
            for t in range(tiles):
                v = [held[i, z, t * SUB:(t + 1) * SUB, :] for i in range(count)]
                for p, (i, j) in enumerate(pairs):
                    accs[p] = accs[p] + v[i] * v[j]
            return tuple(accs)

        accs = lax.fori_loop(start, stop, gram_step, accs)
    lane = lax.broadcasted_iota(jnp.int32, (SUB, nx), 1)
    packed = jnp.zeros((SUB, nx), jnp.float32)
    for p in range(len(pairs)):
        packed = jnp.where(lane == p, jnp.sum(accs[p], axis=1, keepdims=True), packed)
    slots[pl.ds(me, 1)] = jnp.sum(packed, axis=0, keepdims=True).reshape(1, 1, nx)

    pl.semaphore_wait(barrier, total_devices - 1)

    def gram_copy(dx, dy, dz):
        return pltpu.make_async_remote_copy(
            src_ref=slots.at[me],
            dst_ref=slots.at[me],
            send_sem=sent,
            recv_sem=grecv,
            device_id=(gx[dx], gy[dy], gz[dz]),
            device_id_type=MESH,
        )

    for dx, dy, dz in sorted(offsets, key=lambda o: (-(o[0] % 2), order.index(-o[1] % cy))):
        gram_copy(dx, dy, dz).start()

    flat_held = held.reshape(count * ze * ny, nx)

    def all_of(rows, sem):
        part = flat_held.at[pl.ds(0, rows)]
        return pltpu.make_async_remote_copy(
            src_ref=part,
            dst_ref=part,
            send_sem=sem,
            recv_sem=sem,
            device_id=near(0, 0, 1),
            device_id_type=MESH,
        )

    for k, (start, dest, dz) in enumerate(((h, nz + h, -1), (nz, 0, 1))):
        cp = pltpu.make_async_remote_copy(
            src_ref=held.at[:, pl.ds(start, h)],
            dst_ref=held.at[:, pl.ds(dest, h)],
            send_sem=sent,
            recv_sem=zrecv,
            device_id=near(0, 0, dz),
            device_id_type=MESH,
        )
        cp.start()

    def transfer(source, target, recv_sem, dx, dy, dz=0):
        pltpu.make_async_remote_copy(
            src_ref=source,
            dst_ref=target,
            send_sem=sent,
            recv_sem=recv_sem,
            device_id=near(dx, dy, dz),
            device_id_type=MESH,
        ).start()

    third = lane // h

    def gather_x(i, t, rows, head, tail):
        span = slice(t * SUB, (t + 1) * SUB)
        for z in rows:
            v = pltpu.roll(held[i, z, span, :], h * z + h, 1)
            head = jnp.where(third == z + 1, v, head)
            tail = jnp.where(third == z, v, tail)
        raw[i, 0, span, :] = head
        raw[i, 1, span, :] = tail

    def gather_y(i, k, rows):
        start = k * (ny - SUB)
        for z in rows:
            yraw[i, pl.ds(k * SUB * zp + (z - h) % zp, SUB, stride=zp), :] = held[
                i, z, start:start + SUB, :
            ]

    inner, outer = range(h, nz + h), (*range(h), *range(nz + h, ze))

    @pl.loop(0, count)
    def _(i):
        gather_y(i, 1, inner)
        zero = jnp.zeros((SUB, nx), jnp.float32)
        for t in range(tiles):
            gather_x(i, t, inner, zero, zero)

    all_of(2 * count * h * ny, zrecv).wait_recv()
    for i in range(count):
        gather_y(i, 1, outer)

    _, c1, c2, c3 = neighbour_polynomial()

    def by_distance(first, second, square):
        near_by = (c1 + 3.0 * c3) * first + (2.0 * c2) * second + (3.0 * c3) * square
        return near_by, c2 * first + (3.0 * c3) * second

    along = lax.broadcasted_iota(jnp.int32, (zp, nx), 1)
    at_first, at_last = along == 0, along == nx - 1

    def face_sum(d):
        total = jnp.where(at_first, 0.0, pltpu.roll(d, 1, 1))
        total = total + jnp.where(at_last, 0.0, pltpu.roll(d, nx - 1, 1))
        return total + (pltpu.roll(d, 1, 0) + pltpu.roll(d, zp - 1, 0))

    def contribute(i, k):
        d1, d2, d3 = (
            yraw[i, p * zp:(p + 1) * zp, :]
            for p in (range(h) if k == 0 else range(2 * SUB - 1, 2 * SUB - 1 - h, -1))
        )
        m = face_sum(d1)
        mm = face_sum(m) + jnp.where(at_first | at_last, d1, 0.0)
        near_1, near_2 = by_distance(d1[:nz], m[:nz], mm[:nz])
        rows = [
            near_1 + (c2 * d2 + (3.0 * c3) * face_sum(d2))[:nz] + c3 * d3[:nz],
            near_2 + c3 * d2[:nz],
            c3 * d1[:nz],
        ]
        for j, r in enumerate(rows):
            q = j if k == 1 else h - 1 - j
            ycon[k, i, q * nz:(q + 1) * nz, :] = r

    for i in range(count):
        contribute(i, 1)

    odd = lax.rem(iz, 2) == 1
    mate_rows = count * h * nz

    @pl.when(jnp.logical_not(odd))
    def _():
        transfer(ycon.at[1], ymate, mrecv, 0, 0, 1)

    for t in (0, tiles - 1, *range(1, tiles - 1)):
        span = slice(t * SUB, (t + 1) * SUB)
        for i in range(count):
            gather_x(i, t, outer, raw[i, 0, span, :], raw[i, 1, span, :])

    flat_raw = raw.reshape(count * 2 * ny, nx)
    turn = (2, nx - 2)
    far = tuple(
        lax.broadcasted_iota(jnp.int32, (count, nx), 1) % h == c for c in (h - 1, 0)
    )
    for end, (first, second, dy) in enumerate(((ny - 1, ny - 2, 1), (0, 1, -1))):
        for k, dx in enumerate((-1, 1)):
            one, two = (
                flat_raw[pl.ds(k * ny + y, count, stride=2 * ny), :] for y in (first, second)
            )
            cpack[k, end] = jnp.where(far[k], pltpu.roll(two, turn[k], 1), one)
            transfer(cpack.at[k, end], cland.at[1 - k, end], xrecv, dx, dy)

    @pl.loop(0, count)
    def _(i):
        gather_y(i, 0, range(ze))

    for i in range(count):
        contribute(i, 0)

    for p in range(h, SUB):
        mirror = 2 * SUB - 1 - p
        yc[p * zp:(p + 1) * zp, :] = jnp.zeros((zp, nx), jnp.float32)
        yc[mirror * zp:(mirror + 1) * zp, :] = jnp.zeros((zp, nx), jnp.float32)

    @pl.when(odd)
    def _():
        all_of(mate_rows, mrecv).wait_recv()

    all_of(total_devices - 1, grecv).wait_recv()

    total = jnp.sum(slots[...], axis=0)

    g = {}
    for p, (i, j) in enumerate(pairs):
        g[i, j] = jnp.broadcast_to(total[:, p:p + 1], (SUB, nx))
    b = [jnp.ones((SUB, nx), jnp.float32) for _ in range(count)]
    inv = []
    for k in range(count):
        inv.append(1.0 / g[k, k])
        for i in range(k + 1, count):
            f = g[k, i] * inv[k]
            for j in range(i, count):
                g[i, j] = g[i, j] - f * g[k, j]
            b[i] = b[i] - f * b[k]
    solved = [None] * count
    for k in reversed(range(count)):
        solved[k] = b[k] * inv[k]
        for i in range(k):
            b[i] = b[i] - g[i, k] * solved[k]
    norm = solved[0]
    for k in range(1, count):
        norm = norm + solved[k]
    weights = [s / norm for s in solved]

    def blend(parts):
        s = weights[0] * parts(0)
        for i in range(1, count):
            s = s + weights[i] * parts(i)
        return s

    message_rows = h * nz

    def combine_face(target, source):
        for r in range(0, message_rows, SUB):
            target[r:r + SUB, :] = blend(lambda i: source[i, r:r + SUB, :])

    @pl.when(odd)
    def _():
        combine_face(ymix, ymate)
        transfer(ymix, yland.at[0], yrecv, 0, 1, -1)

    for k in range(2):
        for t in range(tiles):
            span = slice(t * SUB, (t + 1) * SUB)
            pack[k, span, :] = blend(lambda i: raw[i, k, span, :])
    for k, dx in enumerate((-1, 1)):
        transfer(pack.at[k], land.at[1 - k, pl.ds(SUB, ny)], xrecv, dx, 0)

    combine_face(ybuf.at[1], ycon.at[1])

    combine_face(ybuf.at[0], ycon.at[0])
    early = jnp.logical_and(iy == 1, jnp.logical_not(odd))

    def send_back():
        transfer(ybuf.at[0], yland.at[1], yrecv, 0, -1)

    pl.when(early)(send_back)

    @pl.loop(0, ze // 2)
    def _(half):
        for r in range(2):
            z = half * 2 + r
            for t in range(tiles):
                span = slice(t * SUB, (t + 1) * SUB)
                comb[z, span, :] = blend(lambda i: held[i, z, span, :])

    row = jnp.zeros((SUB, nx), jnp.float32)
    for k in range(count):
        row = jnp.where(lane == k, weights[k], row)
    wout[...] = row[0:1, :count]

    def around(f, z):
        v = f[z]
        total = pltpu.roll(v, 1, 1) + pltpu.roll(v, nx - 1, 1)
        total = total + (pltpu.roll(v, 1, 0) + pltpu.roll(v, ny - 1, 0))
        return v, total + (f[z - 1] + f[z + 1])

    def planes(start, stop, unroll):
        steps = (stop - start) // unroll

        def wrap(body):
            @pl.loop(0, steps)
            def _(block):
                for r in range(unroll):
                    body(start + block * unroll + r)

            for z in range(start + steps * unroll, stop):
                body(z)
            return body

        return wrap

    alpha, beta, keep, step = sweep_factors()

    @planes(1, ze - 1, UNROLL)
    def _(z):
        v, total = around(comb, z)
        rhs[z] = 6.0 * v - total

    @planes(2, ze - 2, UNROLL)
    def _(z):
        v, total = around(rhs, z)
        it[z] = alpha * v + beta * total

    @pl.when(odd)
    def _():
        transfer(ybuf.at[1], yland.at[0], yrecv, 0, 1)

    pl.when(jnp.logical_not(early))(send_back)

    den_load.wait()

    @planes(h, nz + h, UNROLL)
    def _(z):
        v, total = around(it, z)
        u = keep * v + step * (rhs[z] + total)
        for t in range(tiles):
            span = slice(t * SUB, (t + 1) * SUB)
            base[z - h, span, :] = blend(lambda i: dens[i, z - h, span, :]) + u[span, :]

    wide = ny + 2 * SUB
    inside = slice(SUB, SUB + ny)
    column = lax.broadcasted_iota(jnp.int32, (ny, nx), 1)
    place = column % h

    def plane_sum(d):
        total = pltpu.roll(d, h, 1) + pltpu.roll(d, nx - h, 1)
        return total + (pltpu.roll(d, 1, 0) + pltpu.roll(d, wide - 1, 0))

    all_of(2 * ny + 4 * count, xrecv).wait_recv()
    sub = lax.broadcasted_iota(jnp.int32, (SUB, nx), 0)
    for s in range(2):
        for end, (start, nearest) in enumerate(((0, SUB - 1), (ny + SUB, 0))):
            found = blend(lambda i: jnp.broadcast_to(cland[s, end, i:i + 1, :], (SUB, nx)))
            land[s, start:start + SUB, :] = jnp.where(
                sub == nearest, found, pltpu.roll(found, turn[s], 1)
            )

    sides = []
    for s in range(2):
        own = pack[1 - s]
        d = land[s] - jnp.concatenate([own[ny - SUB:], own, own[:SUB]], axis=0)
        m = plane_sum(d)
        mm = plane_sum(m)
        a1, a2 = by_distance(d[inside], m[inside], mm[inside])
        a3 = c3 * d[inside]
        if s == 0:
            a1, a2, a3 = (pltpu.roll(a, k + 1, 1) for k, a in enumerate((a1, a2, a3)))
            depth = place
        else:
            a1, a2, a3 = (pltpu.roll(a, nx - k - 1, 1) for k, a in enumerate((a1, a2, a3)))
            depth = (h - 1) - place
        sides.append(
            jnp.where(depth == 0, a1, 0.0) + jnp.where(depth <= 1, a2, 0.0) + a3
        )
    even = (column // h) % 2 == 0
    xc[0] = jnp.where(even, sides[1], sides[0])
    xc[1] = jnp.where(even, sides[0], sides[1])

    edge = (lane < h) | (lane >= nx - h)
    for z in range(nz):
        e = z + h
        for t in range(tiles):
            span = slice(t * SUB, (t + 1) * SUB)
            v = pltpu.roll(xc[e % 2, span, :], (-(h * e + h)) % nx, 1)
            base[z, span, :] = base[z, span, :] + jnp.where(edge, v, 0.0)

    all_of(2 * message_rows, yrecv).wait_recv()
    for q in range(h):
        rows = slice(q * nz, (q + 1) * nz)
        for s, p in enumerate((q, 2 * SUB - h + q)):
            yc[p * zp:p * zp + nz, :] = yland[s, rows, :] - ybuf[1 - s, rows, :]

    rows = total_devices - 1 + 2 * count * h * ny + 4 * count + 2 * ny + message_rows

    @pl.when(odd)
    def _():
        all_of(rows + 2 * message_rows, sent).wait_send()

    @pl.when(jnp.logical_not(odd))
    def _():
        all_of(rows + mate_rows, sent).wait_send()


def finish(base, yc, weights, out, wout, stage, sem, wsem):
    nz, ny, nx = base.shape
    zp = yc.shape[0] // (2 * SUB)
    pieces = 4
    per = nz // pieces

    def store(source, target):
        pltpu.make_async_copy(source, target, sem).start()

    wcopy = pltpu.make_async_copy(weights, wout, wsem)
    wcopy.start()
    if ny > 2 * SUB:
        middle = pl.ds(SUB, ny - 2 * SUB)
        store(base.at[:, middle], out.at[:, middle])
    for c in range(pieces):
        part = pl.ds(c * per, per)
        for k, start in enumerate((0, ny - SUB)):
            for z in range(c * per, (c + 1) * per):
                stage[k, z] = base[z, start:start + SUB, :] + yc[
                    pl.ds(k * SUB * zp + z, SUB, stride=zp), :
                ]
            store(stage.at[k, part], out.at[part, pl.ds(start, SUB)])
    pltpu.make_async_copy(base, out, sem).wait()
    wcopy.wait()


def on_device(counts, densities, residuals):
    dims = residuals.shape
    count, nz, ny, nx = dims
    h = SWEEPS
    ze = nz + 2 * h
    zp = pl.cdiv(ze, SUB) * SUB
    n = counts[0] * counts[1] * counts[2]
    chunks = [nz // 8] * 8
    tiles = ny // SUB
    assert tiles >= 2 and h * (ze + 1) <= nx and nz % 8 == 0 and counts[2] % 2 == 0
    dma = pltpu.SemaphoreType.DMA
    f32 = jnp.float32
    field = pltpu.VMEM((ze, ny, nx), f32)

    any_spec = pl.BlockSpec(memory_space=pl.ANY)
    vmem = pl.BlockSpec(memory_space=pltpu.VMEM)
    parts = pl.pallas_call(
        functools.partial(kernel, counts, dims, chunks),
        out_shape=(
            pltpu.VMEM((nz, ny, nx), f32),
            pltpu.VMEM((2 * SUB * zp, nx), f32),
            pltpu.VMEM((1, count), f32),
        ),
        in_specs=[any_spec, any_spec],
        out_specs=(vmem, vmem, vmem),
        scratch_shapes=[
            pltpu.VMEM((count, ze, ny, nx), f32),
            pltpu.VMEM(dims, f32),
            pltpu.VMEM((n, 1, nx), f32),
            field, field, field,
            pltpu.VMEM((count, 2, ny, nx), f32),
            pltpu.VMEM((2, ny, nx), f32),
            pltpu.VMEM((2, ny + 2 * SUB, nx), f32),
            pltpu.VMEM((2, 2, count, nx), f32),
            pltpu.VMEM((2, 2, count, nx), f32),
            pltpu.VMEM((count, 2 * SUB * zp, nx), f32),
            pltpu.VMEM((2, count, h * nz, nx), f32),
            pltpu.VMEM((count, h * nz, nx), f32),
            pltpu.VMEM((h * nz, nx), f32),
            pltpu.VMEM((2, h * nz, nx), f32),
            pltpu.VMEM((2, h * nz, nx), f32),
            pltpu.VMEM((2, ny, nx), f32),
            dma((len(chunks),)), *(dma(()) for _ in range(7)),
        ],
        compiler_params=pltpu.CompilerParams(
            collective_id=0, has_side_effects=True, vmem_limit_bytes=56 * 1024 * 1024
        ),
    )(residuals, densities)
    new_density, weights = pl.pallas_call(
        finish,
        out_shape=(
            jax.ShapeDtypeStruct((nz, ny, nx), f32),
            jax.ShapeDtypeStruct((1, count), f32),
        ),
        in_specs=[vmem, vmem, vmem],
        out_specs=(any_spec, any_spec),
        scratch_shapes=[pltpu.VMEM((2, nz, SUB, nx), f32), dma(()), dma(())],
        compiler_params=pltpu.CompilerParams(vmem_limit_bytes=4 * 1024 * 1024),
    )(*parts)
    return new_density, weights.reshape(count)


def solution(mesh):
    counts = tuple(mesh.shape[a] for a in AXES)
    placed = (P(None, "gz", "gy", "gx"), P(None, "gz", "gy", "gx"))
    return jax.shard_map(
        functools.partial(on_device, counts),
        mesh=mesh,
        in_specs=placed,
        out_specs=(P("gz", "gy", "gx"), P()),
        check_vma=False,
    )
```

```python
import functools
import math

import jax
import jax.numpy as jnp
from jax import lax
from jax.experimental import pallas as pl
from jax.experimental.pallas import tpu as pltpu
from jax.sharding import PartitionSpec as P

MESH = pl.DeviceIdType.MESH
SWEEPS = 3
SUB = 8
UNROLL = 12
shift_value = 0.15
mix_amount = 0.7
AXES = ("gx", "gy", "gz")


def sweep_weights():
    diag_value = 6.0 + shift_value
    upper = (shift_value + 12.0) / diag_value
    lower = upper / 3.0
    return [
        1.0
        / (
            (upper + lower) / 2.0
            + (upper - lower) / 2.0 * math.cos(math.pi * (2 * k - 1) / (2 * SWEEPS))
        )
        for k in range(1, SWEEPS + 1)
    ]


def sweep_factors():
    diag_value = 6.0 + shift_value
    w1, w2, w3 = sweep_weights()
    alpha = ((1.0 - w2) * w1 + w2) / diag_value
    beta = w1 * w2 / (diag_value * diag_value)
    return alpha, beta, mix_amount * (1.0 - w3), mix_amount * w3 / diag_value


def neighbour_polynomial():
    alpha, beta, keep, step = sweep_factors()
    q0 = keep * alpha + step
    q1 = keep * beta + step * alpha
    q2 = step * beta
    return 6.0 * q0, 6.0 * q1 - q0, 6.0 * q2 - q1, -q2


def kernel(
    counts, dims, chunks,
    res, den, base, yc, wout,
    held, dens, slots, comb, rhs, it, raw, pack, land, cpack, cland,
    yraw, ycon, ymate, ymix, ybuf, yland, xc,
    in_sem, den_sem, sent, grecv, zrecv, mrecv, xrecv, yrecv,
):
    count, nz, ny, nx = dims
    cx, cy, cz = counts
    total_devices = cx * cy * cz
    h = SWEEPS
    ze = nz + 2 * h
    zp = yraw.shape[1] // (2 * SUB)
    tiles = ny // SUB
    ix, iy, iz = (lax.axis_index(a) for a in AXES)
    me = (ix * cy + iy) * cz + iz

    def near(dx, dy, dz):
        return (
            lax.rem(ix + dx + cx, cx),
            lax.rem(iy + dy + cy, cy),
            lax.rem(iz + dz + cz, cz),
        )

    loads, first = [], 0
    for c, size in enumerate(chunks):
        cp = pltpu.make_async_copy(
            res.at[:, pl.ds(first, size)], held.at[:, pl.ds(h + first, size)], in_sem.at[c]
        )
        cp.start()
        loads.append((cp, h + first, h + first + size))
        first += size

    barrier = pltpu.get_barrier_semaphore()

    offsets = [
        (dx, dy, dz) for dx in range(cx) for dy in range(cy) for dz in range(cz) if dx or dy or dz
    ]
    order = [1, cy - 1, *range(2, cy - 1), 0]
    offsets.sort(key=lambda o: (order.index(o[1]), -(o[0] % 2)))
    gx = [lax.rem(ix + d, cx) for d in range(cx)]
    gy = [lax.rem(iy + d, cy) for d in range(cy)]
    gz = [lax.rem(iz + d, cz) for d in range(cz)]
    for dx, dy, dz in offsets:
        pl.semaphore_signal(
            barrier, inc=1, device_id=(gx[dx], gy[dy], gz[dz]), device_id_type=MESH
        )

    pairs = [(i, j) for i in range(count) for j in range(i, count)]
    accs = tuple(jnp.zeros((SUB, nx), jnp.float32) for _ in pairs)
    den_load = pltpu.make_async_copy(den, dens, den_sem)
    for c, (load, start, stop) in enumerate(loads):
        load.wait()
        if c == len(loads) - 1:
            den_load.start()

        def gram_step(z, accs):
            accs = list(accs)
            for t in range(tiles):
                v = [held[i, z, t * SUB:(t + 1) * SUB, :] for i in range(count)]
                for p, (i, j) in enumerate(pairs):
                    accs[p] = accs[p] + v[i] * v[j]
            return tuple(accs)

        accs = lax.fori_loop(start, stop, gram_step, accs)
    lane = lax.broadcasted_iota(jnp.int32, (SUB, nx), 1)
    packed = jnp.zeros((SUB, nx), jnp.float32)
    for p in range(len(pairs)):
        packed = jnp.where(lane == p, jnp.sum(accs[p], axis=1, keepdims=True), packed)
    slots[pl.ds(me, 1)] = jnp.sum(packed, axis=0, keepdims=True).reshape(1, 1, nx)

    pl.semaphore_wait(barrier, total_devices - 1)

    def gram_copy(dx, dy, dz):
        return pltpu.make_async_remote_copy(
            src_ref=slots.at[me],
            dst_ref=slots.at[me],
            send_sem=sent,
            recv_sem=grecv,
            device_id=(gx[dx], gy[dy], gz[dz]),
            device_id_type=MESH,
        )

    for dx, dy, dz in sorted(offsets, key=lambda o: (-(o[0] % 2), order.index(-o[1] % cy))):
        gram_copy(dx, dy, dz).start()

    flat_held = held.reshape(count * ze * ny, nx)

    def all_of(rows, sem):
        part = flat_held.at[pl.ds(0, rows)]
        return pltpu.make_async_remote_copy(
            src_ref=part,
            dst_ref=part,
            send_sem=sem,
            recv_sem=sem,
            device_id=near(0, 0, 1),
            device_id_type=MESH,
        )

    for k, (start, dest, dz) in enumerate(((h, nz + h, -1), (nz, 0, 1))):
        cp = pltpu.make_async_remote_copy(
            src_ref=held.at[:, pl.ds(start, h)],
            dst_ref=held.at[:, pl.ds(dest, h)],
            send_sem=sent,
            recv_sem=zrecv,
            device_id=near(0, 0, dz),
            device_id_type=MESH,
        )
        cp.start()

    def transfer(source, target, recv_sem, dx, dy, dz=0):
        pltpu.make_async_remote_copy(
            src_ref=source,
            dst_ref=target,
            send_sem=sent,
            recv_sem=recv_sem,
            device_id=near(dx, dy, dz),
            device_id_type=MESH,
        ).start()

    third = lane // h

    def gather_x(i, t, rows, head, tail):
        span = slice(t * SUB, (t + 1) * SUB)
        for z in rows:
            v = pltpu.roll(held[i, z, span, :], h * z + h, 1)
            head = jnp.where(third == z + 1, v, head)
            tail = jnp.where(third == z, v, tail)
        raw[i, 0, span, :] = head
        raw[i, 1, span, :] = tail

    def gather_y(i, k, rows):
        start = k * (ny - SUB)
        for z in rows:
            yraw[i, pl.ds(k * SUB * zp + (z - h) % zp, SUB, stride=zp), :] = held[
                i, z, start:start + SUB, :
            ]

    inner, outer = range(h, nz + h), (*range(h), *range(nz + h, ze))

    @pl.loop(0, count)
    def _(i):
        gather_y(i, 1, inner)
        zero = jnp.zeros((SUB, nx), jnp.float32)
        for t in range(tiles):
            gather_x(i, t, inner, zero, zero)

    all_of(2 * count * h * ny, zrecv).wait_recv()
    for i in range(count):
        gather_y(i, 1, outer)

    _, c1, c2, c3 = neighbour_polynomial()

    def by_distance(first, second, square):
        near_by = (c1 + 3.0 * c3) * first + (2.0 * c2) * second + (3.0 * c3) * square
        return near_by, c2 * first + (3.0 * c3) * second

    along = lax.broadcasted_iota(jnp.int32, (zp, nx), 1)
    at_first, at_last = along == 0, along == nx - 1

    def face_sum(d):
        total = jnp.where(at_first, 0.0, pltpu.roll(d, 1, 1))
        total = total + jnp.where(at_last, 0.0, pltpu.roll(d, nx - 1, 1))
        return total + (pltpu.roll(d, 1, 0) + pltpu.roll(d, zp - 1, 0))

    def contribute(i, k):
        d1, d2, d3 = (
            yraw[i, p * zp:(p + 1) * zp, :]
            for p in (range(h) if k == 0 else range(2 * SUB - 1, 2 * SUB - 1 - h, -1))
        )
        m = face_sum(d1)
        mm = face_sum(m) + jnp.where(at_first | at_last, d1, 0.0)
        near_1, near_2 = by_distance(d1[:nz], m[:nz], mm[:nz])
        rows = [
            near_1 + (c2 * d2 + (3.0 * c3) * face_sum(d2))[:nz] + c3 * d3[:nz],
            near_2 + c3 * d2[:nz],
            c3 * d1[:nz],
        ]
        for j, r in enumerate(rows):
            q = j if k == 1 else h - 1 - j
            ycon[k, i, q * nz:(q + 1) * nz, :] = r

    for i in range(count):
        contribute(i, 1)

    odd = lax.rem(iz, 2) == 1
    mate_rows = count * h * nz

    @pl.when(jnp.logical_not(odd))
    def _():
        transfer(ycon.at[1], ymate, mrecv, 0, 0, 1)

    for t in (0, tiles - 1, *range(1, tiles - 1)):
        span = slice(t * SUB, (t + 1) * SUB)
        for i in range(count):
            gather_x(i, t, outer, raw[i, 0, span, :], raw[i, 1, span, :])

    flat_raw = raw.reshape(count * 2 * ny, nx)
    turn = (2, nx - 2)
    far = tuple(
        lax.broadcasted_iota(jnp.int32, (count, nx), 1) % h == c for c in (h - 1, 0)
    )
    for end, (first, second, dy) in enumerate(((ny - 1, ny - 2, 1), (0, 1, -1))):
        for k, dx in enumerate((-1, 1)):
            one, two = (
                flat_raw[pl.ds(k * ny + y, count, stride=2 * ny), :] for y in (first, second)
            )
            cpack[k, end] = jnp.where(far[k], pltpu.roll(two, turn[k], 1), one)
            transfer(cpack.at[k, end], cland.at[1 - k, end], xrecv, dx, dy)

    @pl.loop(0, count)
    def _(i):
        gather_y(i, 0, range(ze))

    for i in range(count):
        contribute(i, 0)

    for p in range(h, SUB):
        mirror = 2 * SUB - 1 - p
        yc[p * zp:(p + 1) * zp, :] = jnp.zeros((zp, nx), jnp.float32)
        yc[mirror * zp:(mirror + 1) * zp, :] = jnp.zeros((zp, nx), jnp.float32)

    @pl.when(odd)
    def _():
        all_of(mate_rows, mrecv).wait_recv()

    all_of(total_devices - 1, grecv).wait_recv()

    parts = [slots[k] for k in range(total_devices)]
    while len(parts) > 1:
        parts = [sum(parts[k + 1:k + 2], parts[k]) for k in range(0, len(parts), 2)]
    total = parts[0]

    g = {}
    for p, (i, j) in enumerate(pairs):
        g[i, j] = jnp.broadcast_to(total[:, p:p + 1], (SUB, nx))
    b = [jnp.ones((SUB, nx), jnp.float32) for _ in range(count)]
    inv = []
    for k in range(count):
        inv.append(1.0 / g[k, k])
        for i in range(k + 1, count):
            f = g[k, i] * inv[k]
            for j in range(i, count):
                g[i, j] = g[i, j] - f * g[k, j]
            b[i] = b[i] - f * b[k]
    solved = [None] * count
    for k in reversed(range(count)):
        solved[k] = b[k] * inv[k]
        for i in range(k):
            b[i] = b[i] - g[i, k] * solved[k]
    norm = solved[0]
    for k in range(1, count):
        norm = norm + solved[k]
    scale = 1.0 / norm
    weights = [s * scale for s in solved]

    def blend(parts):
        s = weights[0] * parts(0)
        for i in range(1, count):
            s = s + weights[i] * parts(i)
        return s

    message_rows = h * nz

    def combine_face(target, source):
        for r in range(0, message_rows, SUB):
            target[r:r + SUB, :] = blend(lambda i: source[i, r:r + SUB, :])

    @pl.when(odd)
    def _():
        combine_face(ymix, ymate)
        transfer(ymix, yland.at[0], yrecv, 0, 1, -1)

    for k in range(2):
        for t in range(tiles):
            span = slice(t * SUB, (t + 1) * SUB)
            pack[k, span, :] = blend(lambda i: raw[i, k, span, :])
    for k, dx in enumerate((-1, 1)):
        transfer(pack.at[k], land.at[1 - k, pl.ds(SUB, ny)], xrecv, dx, 0)

    combine_face(ybuf.at[1], ycon.at[1])

    combine_face(ybuf.at[0], ycon.at[0])
    early = jnp.logical_and(iy == 1, jnp.logical_not(odd))

    def send_back():
        transfer(ybuf.at[0], yland.at[1], yrecv, 0, -1)

    pl.when(early)(send_back)

    @pl.loop(0, ze // 2)
    def _(half):
        for r in range(2):
            z = half * 2 + r
            for t in range(tiles):
                span = slice(t * SUB, (t + 1) * SUB)
                comb[z, span, :] = blend(lambda i: held[i, z, span, :])

    row = jnp.zeros((SUB, nx), jnp.float32)
    for k in range(count):
        row = jnp.where(lane == k, weights[k], row)
    wout[...] = row[0:1, :count]

    def around(f, z):
        v = f[z]
        total = pltpu.roll(v, 1, 1) + pltpu.roll(v, nx - 1, 1)
        total = total + (pltpu.roll(v, 1, 0) + pltpu.roll(v, ny - 1, 0))
        return v, total + (f[z - 1] + f[z + 1])

    def planes(start, stop, unroll):
        steps = (stop - start) // unroll

        def wrap(body):
            @pl.loop(0, steps)
            def _(block):
                for r in range(unroll):
                    body(start + block * unroll + r)

            for z in range(start + steps * unroll, stop):
                body(z)
            return body

        return wrap

    alpha, beta, keep, step = sweep_factors()

    @planes(1, ze - 1, UNROLL)
    def _(z):
        v, total = around(comb, z)
        rhs[z] = 6.0 * v - total

    def second_pass(z):
        v, total = around(rhs, z)
        it[z] = alpha * v + beta * total

    planes(2, 2 + 12, UNROLL)(second_pass)

    @pl.when(odd)
    def _():
        transfer(ybuf.at[1], yland.at[0], yrecv, 0, 1)

    planes(2 + 12, ze - 2, UNROLL)(second_pass)

    pl.when(jnp.logical_not(early))(send_back)

    den_load.wait()

    @planes(h, nz + h, UNROLL)
    def _(z):
        v, total = around(it, z)
        u = keep * v + step * (rhs[z] + total)
        for t in range(tiles):
            span = slice(t * SUB, (t + 1) * SUB)
            base[z - h, span, :] = blend(lambda i: dens[i, z - h, span, :]) + u[span, :]

    wide = ny + 2 * SUB
    inside = slice(SUB, SUB + ny)
    column = lax.broadcasted_iota(jnp.int32, (ny, nx), 1)
    place = column % h

    def plane_sum(d):
        total = pltpu.roll(d, h, 1) + pltpu.roll(d, nx - h, 1)
        return total + (pltpu.roll(d, 1, 0) + pltpu.roll(d, wide - 1, 0))

    all_of(2 * ny + 4 * count, xrecv).wait_recv()
    sub = lax.broadcasted_iota(jnp.int32, (SUB, nx), 0)
    for s in range(2):
        for end, (start, nearest) in enumerate(((0, SUB - 1), (ny + SUB, 0))):
            found = blend(lambda i: jnp.broadcast_to(cland[s, end, i:i + 1, :], (SUB, nx)))
            land[s, start:start + SUB, :] = jnp.where(
                sub == nearest, found, pltpu.roll(found, turn[s], 1)
            )

    sides = []
    for s in range(2):
        own = pack[1 - s]
        d = land[s] - jnp.concatenate([own[ny - SUB:], own, own[:SUB]], axis=0)
        m = plane_sum(d)
        mm = plane_sum(m)
        a1, a2 = by_distance(d[inside], m[inside], mm[inside])
        a3 = c3 * d[inside]
        if s == 0:
            a1, a2, a3 = (pltpu.roll(a, k + 1, 1) for k, a in enumerate((a1, a2, a3)))
            depth = place
        else:
            a1, a2, a3 = (pltpu.roll(a, nx - k - 1, 1) for k, a in enumerate((a1, a2, a3)))
            depth = (h - 1) - place
        sides.append(
            jnp.where(depth == 0, a1, 0.0) + jnp.where(depth <= 1, a2, 0.0) + a3
        )
    even = (column // h) % 2 == 0
    xc[0] = jnp.where(even, sides[1], sides[0])
    xc[1] = jnp.where(even, sides[0], sides[1])

    edge = (lane < h) | (lane >= nx - h)
    for z in range(nz):
        e = z + h
        for t in range(tiles):
            span = slice(t * SUB, (t + 1) * SUB)
            v = pltpu.roll(xc[e % 2, span, :], (-(h * e + h)) % nx, 1)
            base[z, span, :] = base[z, span, :] + jnp.where(edge, v, 0.0)

    all_of(2 * message_rows, yrecv).wait_recv()
    for q in range(h):
        rows = slice(q * nz, (q + 1) * nz)
        for s, p in enumerate((q, 2 * SUB - h + q)):
            yc[p * zp:p * zp + nz, :] = yland[s, rows, :] - ybuf[1 - s, rows, :]

    rows = total_devices - 1 + 2 * count * h * ny + 4 * count + 2 * ny + message_rows

    @pl.when(odd)
    def _():
        all_of(rows + 2 * message_rows, sent).wait_send()

    @pl.when(jnp.logical_not(odd))
    def _():
        all_of(rows + mate_rows, sent).wait_send()


def finish(base, yc, weights, out, wout, stage, sem, wsem):
    nz, ny, nx = base.shape
    zp = yc.shape[0] // (2 * SUB)
    pieces = 4
    per = nz // pieces

    def store(source, target):
        pltpu.make_async_copy(source, target, sem).start()

    wcopy = pltpu.make_async_copy(weights, wout, wsem)
    wcopy.start()
    if ny > 2 * SUB:
        middle = pl.ds(SUB, ny - 2 * SUB)
        store(base.at[:, middle], out.at[:, middle])
    for c in range(pieces):
        part = pl.ds(c * per, per)
        for k, start in enumerate((0, ny - SUB)):
            for z in range(c * per, (c + 1) * per):
                stage[k, z] = base[z, start:start + SUB, :] + yc[
                    pl.ds(k * SUB * zp + z, SUB, stride=zp), :
                ]
            store(stage.at[k, part], out.at[part, pl.ds(start, SUB)])
    pltpu.make_async_copy(base, out, sem).wait()
    wcopy.wait()


def on_device(counts, densities, residuals):
    dims = residuals.shape
    count, nz, ny, nx = dims
    h = SWEEPS
    ze = nz + 2 * h
    zp = pl.cdiv(ze, SUB) * SUB
    n = counts[0] * counts[1] * counts[2]
    chunks = [nz // 8] * 8
    tiles = ny // SUB
    assert tiles >= 2 and h * (ze + 1) <= nx and nz % 8 == 0 and counts[2] % 2 == 0
    dma = pltpu.SemaphoreType.DMA
    f32 = jnp.float32
    field = pltpu.VMEM((ze, ny, nx), f32)

    any_spec = pl.BlockSpec(memory_space=pl.ANY)
    vmem = pl.BlockSpec(memory_space=pltpu.VMEM)
    parts = pl.pallas_call(
        functools.partial(kernel, counts, dims, chunks),
        out_shape=(
            pltpu.VMEM((nz, ny, nx), f32),
            pltpu.VMEM((2 * SUB * zp, nx), f32),
            pltpu.VMEM((1, count), f32),
        ),
        in_specs=[any_spec, any_spec],
        out_specs=(vmem, vmem, vmem),
        scratch_shapes=[
            pltpu.VMEM((count, ze, ny, nx), f32),
            pltpu.VMEM(dims, f32),
            pltpu.VMEM((n, 1, nx), f32),
            field, field, field,
            pltpu.VMEM((count, 2, ny, nx), f32),
            pltpu.VMEM((2, ny, nx), f32),
            pltpu.VMEM((2, ny + 2 * SUB, nx), f32),
            pltpu.VMEM((2, 2, count, nx), f32),
            pltpu.VMEM((2, 2, count, nx), f32),
            pltpu.VMEM((count, 2 * SUB * zp, nx), f32),
            pltpu.VMEM((2, count, h * nz, nx), f32),
            pltpu.VMEM((count, h * nz, nx), f32),
            pltpu.VMEM((h * nz, nx), f32),
            pltpu.VMEM((2, h * nz, nx), f32),
            pltpu.VMEM((2, h * nz, nx), f32),
            pltpu.VMEM((2, ny, nx), f32),
            dma((len(chunks),)), *(dma(()) for _ in range(7)),
        ],
        compiler_params=pltpu.CompilerParams(
            collective_id=0, has_side_effects=True, vmem_limit_bytes=56 * 1024 * 1024
        ),
    )(residuals, densities)
    new_density, weights = pl.pallas_call(
        finish,
        out_shape=(
            jax.ShapeDtypeStruct((nz, ny, nx), f32),
            jax.ShapeDtypeStruct((1, count), f32),
        ),
        in_specs=[vmem, vmem, vmem],
        out_specs=(any_spec, any_spec),
        scratch_shapes=[pltpu.VMEM((2, nz, SUB, nx), f32), dma(()), dma(())],
        compiler_params=pltpu.CompilerParams(vmem_limit_bytes=4 * 1024 * 1024),
    )(*parts)
    return new_density, weights.reshape(count)


def solution(mesh):
    counts = tuple(mesh.shape[a] for a in AXES)
    placed = (P(None, "gz", "gy", "gx"), P(None, "gz", "gy", "gx"))
    return jax.shard_map(
        functools.partial(on_device, counts),
        mesh=mesh,
        in_specs=placed,
        out_specs=(P("gz", "gy", "gx"), P()),
        check_vma=False,
    )
```

```python
import functools
import math

import jax
import jax.numpy as jnp
from jax import lax
from jax.experimental import pallas as pl
from jax.experimental.pallas import tpu as pltpu
from jax.sharding import PartitionSpec as P

MESH = pl.DeviceIdType.MESH
SWEEPS = 3
SUB = 8
UNROLL = 12
shift_value = 0.15
mix_amount = 0.7
AXES = ("gx", "gy", "gz")


def sweep_weights():
    diag_value = 6.0 + shift_value
    upper = (shift_value + 12.0) / diag_value
    lower = upper / 3.0
    return [
        1.0
        / (
            (upper + lower) / 2.0
            + (upper - lower) / 2.0 * math.cos(math.pi * (2 * k - 1) / (2 * SWEEPS))
        )
        for k in range(1, SWEEPS + 1)
    ]


def sweep_factors():
    diag_value = 6.0 + shift_value
    w1, w2, w3 = sweep_weights()
    alpha = ((1.0 - w2) * w1 + w2) / diag_value
    beta = w1 * w2 / (diag_value * diag_value)
    return alpha, beta, mix_amount * (1.0 - w3), mix_amount * w3 / diag_value


def neighbour_polynomial():
    alpha, beta, keep, step = sweep_factors()
    q0 = keep * alpha + step
    q1 = keep * beta + step * alpha
    q2 = step * beta
    return 6.0 * q0, 6.0 * q1 - q0, 6.0 * q2 - q1, -q2


def kernel(
    counts, dims, chunks,
    res, den, base, yc, wout,
    held, dens, slots, comb, rhs, it, raw, pack, land, cpack, cland,
    yraw, ycon, ymate, ymix, ybuf, yland, xc,
    in_sem, den_sem, sent, grecv, zrecv, mrecv, xrecv, yrecv,
):
    count, nz, ny, nx = dims
    cx, cy, cz = counts
    total_devices = cx * cy * cz
    h = SWEEPS
    ze = nz + 2 * h
    zp = yraw.shape[1] // (2 * SUB)
    tiles = ny // SUB
    ix, iy, iz = (lax.axis_index(a) for a in AXES)
    me = (ix * cy + iy) * cz + iz

    def near(dx, dy, dz):
        return (
            lax.rem(ix + dx + cx, cx),
            lax.rem(iy + dy + cy, cy),
            lax.rem(iz + dz + cz, cz),
        )

    loads, first = [], 0
    for c, size in enumerate(chunks):
        cp = pltpu.make_async_copy(
            res.at[:, pl.ds(first, size)], held.at[:, pl.ds(h + first, size)], in_sem.at[c]
        )
        cp.start()
        loads.append((cp, h + first, h + first + size))
        first += size

    barrier = pltpu.get_barrier_semaphore()

    offsets = [
        (dx, dy, dz) for dx in range(cx) for dy in range(cy) for dz in range(cz) if dx or dy or dz
    ]
    order = [1, cy - 1, *range(2, cy - 1), 0]
    offsets.sort(key=lambda o: (order.index(o[1]), -(o[0] % 2)))
    gx = [lax.rem(ix + d, cx) for d in range(cx)]
    gy = [lax.rem(iy + d, cy) for d in range(cy)]
    gz = [lax.rem(iz + d, cz) for d in range(cz)]
    for dx, dy, dz in offsets:
        pl.semaphore_signal(
            barrier, inc=1, device_id=(gx[dx], gy[dy], gz[dz]), device_id_type=MESH
        )

    pairs = [(i, j) for i in range(count) for j in range(i, count)]
    accs = tuple(jnp.zeros((SUB, nx), jnp.float32) for _ in pairs)
    den_load = pltpu.make_async_copy(den, dens, den_sem)
    for c, (load, start, stop) in enumerate(loads):
        load.wait()
        if c == len(loads) - 1:
            den_load.start()

        def gram_step(z, accs):
            accs = list(accs)
            for t in range(tiles):
                v = [held[i, z, t * SUB:(t + 1) * SUB, :] for i in range(count)]
                for p, (i, j) in enumerate(pairs):
                    accs[p] = accs[p] + v[i] * v[j]
            return tuple(accs)

        accs = lax.fori_loop(start, stop, gram_step, accs)
    lane = lax.broadcasted_iota(jnp.int32, (SUB, nx), 1)
    packed = jnp.zeros((SUB, nx), jnp.float32)
    for p in range(len(pairs)):
        packed = jnp.where(lane == p, jnp.sum(accs[p], axis=1, keepdims=True), packed)
    slots[pl.ds(me, 1)] = jnp.sum(packed, axis=0, keepdims=True).reshape(1, 1, nx)

    pl.semaphore_wait(barrier, total_devices - 1)

    def gram_copy(dx, dy, dz):
        return pltpu.make_async_remote_copy(
            src_ref=slots.at[me],
            dst_ref=slots.at[me],
            send_sem=sent,
            recv_sem=grecv,
            device_id=(gx[dx], gy[dy], gz[dz]),
            device_id_type=MESH,
        )

    for dx, dy, dz in sorted(offsets, key=lambda o: -sum(min(d, c - d) for d, c in zip(o, counts))):
        gram_copy(dx, dy, dz).start()

    flat_held = held.reshape(count * ze * ny, nx)

    def all_of(rows, sem):
        part = flat_held.at[pl.ds(0, rows)]
        return pltpu.make_async_remote_copy(
            src_ref=part,
            dst_ref=part,
            send_sem=sem,
            recv_sem=sem,
            device_id=near(0, 0, 1),
            device_id_type=MESH,
        )

    def transfer(source, target, recv_sem, dx, dy, dz=0):
        pltpu.make_async_remote_copy(
            src_ref=source,
            dst_ref=target,
            send_sem=sent,
            recv_sem=recv_sem,
            device_id=near(dx, dy, dz),
            device_id_type=MESH,
        ).start()

    third = lane // h

    def gather_x(i, t, rows, head, tail):
        span = slice(t * SUB, (t + 1) * SUB)
        for z in rows:
            v = pltpu.roll(held[i, z, span, :], h * z + h, 1)
            head = jnp.where(third == z + 1, v, head)
            tail = jnp.where(third == z, v, tail)
        raw[i, 0, span, :] = head
        raw[i, 1, span, :] = tail

    def gather_y(i, k, rows):
        start = k * (ny - SUB)
        for z in rows:
            yraw[i, pl.ds(k * SUB * zp + (z - h) % zp, SUB, stride=zp), :] = held[
                i, z, start:start + SUB, :
            ]

    inner, outer = range(h, nz + h), (*range(h), *range(nz + h, ze))

    def gather_inner(i):
        gather_y(i, 1, inner)
        zero = jnp.zeros((SUB, nx), jnp.float32)
        for t in range(tiles):
            gather_x(i, t, inner, zero, zero)

    pl.loop(0, 1)(gather_inner)

    for k, (start, dest, dz) in enumerate(((h, nz + h, -1), (nz, 0, 1))):
        cp = pltpu.make_async_remote_copy(
            src_ref=held.at[:, pl.ds(start, h)],
            dst_ref=held.at[:, pl.ds(dest, h)],
            send_sem=sent,
            recv_sem=zrecv,
            device_id=near(0, 0, dz),
            device_id_type=MESH,
        )
        cp.start()

    pl.loop(1, count)(gather_inner)

    all_of(2 * count * h * ny, zrecv).wait_recv()
    for i in range(count):
        gather_y(i, 1, outer)

    _, c1, c2, c3 = neighbour_polynomial()

    def by_distance(first, second, square):
        near_by = (c1 + 3.0 * c3) * first + (2.0 * c2) * second + (3.0 * c3) * square
        return near_by, c2 * first + (3.0 * c3) * second

    along = lax.broadcasted_iota(jnp.int32, (zp, nx), 1)
    at_first, at_last = along == 0, along == nx - 1

    def face_sum(d):
        total = jnp.where(at_first, 0.0, pltpu.roll(d, 1, 1))
        total = total + jnp.where(at_last, 0.0, pltpu.roll(d, nx - 1, 1))
        return total + (pltpu.roll(d, 1, 0) + pltpu.roll(d, zp - 1, 0))

    def contribute(i, k):
        d1, d2, d3 = (
            yraw[i, p * zp:(p + 1) * zp, :]
            for p in (range(h) if k == 0 else range(2 * SUB - 1, 2 * SUB - 1 - h, -1))
        )
        m = face_sum(d1)
        mm = face_sum(m) + jnp.where(at_first | at_last, d1, 0.0)
        near_1, near_2 = by_distance(d1[:nz], m[:nz], mm[:nz])
        rows = [
            near_1 + (c2 * d2 + (3.0 * c3) * face_sum(d2))[:nz] + c3 * d3[:nz],
            near_2 + c3 * d2[:nz],
            c3 * d1[:nz],
        ]
        for j, r in enumerate(rows):
            q = j if k == 1 else h - 1 - j
            ycon[k, i, q * nz:(q + 1) * nz, :] = r

    for i in range(count):
        contribute(i, 1)

    odd = lax.rem(iz, 2) == 1
    mate_rows = count * h * nz

    @pl.when(jnp.logical_not(odd))
    def _():
        transfer(ycon.at[1], ymate, mrecv, 0, 0, 1)

    for t in (0, tiles - 1, *range(1, tiles - 1)):
        span = slice(t * SUB, (t + 1) * SUB)
        for i in range(count):
            gather_x(i, t, outer, raw[i, 0, span, :], raw[i, 1, span, :])

    flat_raw = raw.reshape(count * 2 * ny, nx)
    turn = (2, nx - 2)
    far = tuple(
        lax.broadcasted_iota(jnp.int32, (count, nx), 1) % h == c for c in (h - 1, 0)
    )
    for end, (first, second, dy) in enumerate(((ny - 1, ny - 2, 1), (0, 1, -1))):
        for k, dx in enumerate((-1, 1)):
            one, two = (
                flat_raw[pl.ds(k * ny + y, count, stride=2 * ny), :] for y in (first, second)
            )
            cpack[k, end] = jnp.where(far[k], pltpu.roll(two, turn[k], 1), one)
            transfer(cpack.at[k, end], cland.at[1 - k, end], xrecv, dx, dy)

    @pl.loop(0, count)
    def _(i):
        gather_y(i, 0, range(ze))

    for i in range(count):
        contribute(i, 0)

    for p in range(h, SUB):
        mirror = 2 * SUB - 1 - p
        yc[p * zp:(p + 1) * zp, :] = jnp.zeros((zp, nx), jnp.float32)
        yc[mirror * zp:(mirror + 1) * zp, :] = jnp.zeros((zp, nx), jnp.float32)

    @pl.when(odd)
    def _():
        all_of(mate_rows, mrecv).wait_recv()

    all_of(total_devices - 1, grecv).wait_recv()

    parts = [slots[k] for k in range(total_devices)]
    while len(parts) > 1:
        parts = [sum(parts[k + 1:k + 2], parts[k]) for k in range(0, len(parts), 2)]
    total = parts[0]

    g = {}
    for p, (i, j) in enumerate(pairs):
        g[i, j] = jnp.broadcast_to(total[:, p:p + 1], (SUB, nx))
    b = [jnp.ones((SUB, nx), jnp.float32) for _ in range(count)]
    inv = []
    for k in range(count):
        inv.append(1.0 / g[k, k])
        for i in range(k + 1, count):
            f = g[k, i] * inv[k]
            for j in range(i, count):
                g[i, j] = g[i, j] - f * g[k, j]
            b[i] = b[i] - f * b[k]
    solved = [None] * count
    for k in reversed(range(count)):
        solved[k] = b[k] * inv[k]
        for i in range(k):
            b[i] = b[i] - g[i, k] * solved[k]
    norm = solved[0]
    for k in range(1, count):
        norm = norm + solved[k]
    scale = 1.0 / norm
    weights = [s * scale for s in solved]

    def blend(parts):
        s = weights[0] * parts(0)
        for i in range(1, count):
            s = s + weights[i] * parts(i)
        return s

    message_rows = h * nz

    def combine_face(target, source):
        for r in range(0, message_rows, SUB):
            target[r:r + SUB, :] = blend(lambda i: source[i, r:r + SUB, :])

    @pl.when(odd)
    def _():
        combine_face(ymix, ymate)
        transfer(ymix, yland.at[0], yrecv, 0, 1, -1)

    for k in range(2):
        for t in range(tiles):
            span = slice(t * SUB, (t + 1) * SUB)
            pack[k, span, :] = blend(lambda i: raw[i, k, span, :])
    for k, dx in enumerate((-1, 1)):
        transfer(pack.at[k], land.at[1 - k, pl.ds(SUB, ny)], xrecv, dx, 0)

    combine_face(ybuf.at[1], ycon.at[1])

    combine_face(ybuf.at[0], ycon.at[0])
    early = jnp.logical_and(iy == 1, jnp.logical_not(odd))

    def send_back():
        transfer(ybuf.at[0], yland.at[1], yrecv, 0, -1)

    pl.when(early)(send_back)

    @pl.loop(0, ze // 2)
    def _(half):
        for r in range(2):
            z = half * 2 + r
            for t in range(tiles):
                span = slice(t * SUB, (t + 1) * SUB)
                comb[z, span, :] = blend(lambda i: held[i, z, span, :])

    row = jnp.zeros((SUB, nx), jnp.float32)
    for k in range(count):
        row = jnp.where(lane == k, weights[k], row)
    wout[...] = row[0:1, :count]

    def around(f, z):
        v = f[z]
        total = pltpu.roll(v, 1, 1) + pltpu.roll(v, nx - 1, 1)
        total = total + (pltpu.roll(v, 1, 0) + pltpu.roll(v, ny - 1, 0))
        return v, total + (f[z - 1] + f[z + 1])

    def planes(start, stop, unroll):
        steps = (stop - start) // unroll

        def wrap(body):
            @pl.loop(0, steps)
            def _(block):
                for r in range(unroll):
                    body(start + block * unroll + r)

            for z in range(start + steps * unroll, stop):
                body(z)
            return body

        return wrap

    alpha, beta, keep, step = sweep_factors()

    @planes(1, ze - 1, UNROLL)
    def _(z):
        v, total = around(comb, z)
        rhs[z] = 6.0 * v - total

    def second_pass(z):
        v, total = around(rhs, z)
        it[z] = alpha * v + beta * total

    planes(2, 2 + 12, UNROLL)(second_pass)

    @pl.when(odd)
    def _():
        transfer(ybuf.at[1], yland.at[0], yrecv, 0, 1)

    planes(2 + 12, ze - 2, UNROLL)(second_pass)

    pl.when(jnp.logical_not(early))(send_back)

    den_load.wait()

    @planes(h, nz + h, UNROLL)
    def _(z):
        v, total = around(it, z)
        u = keep * v + step * (rhs[z] + total)
        for t in range(tiles):
            span = slice(t * SUB, (t + 1) * SUB)
            base[z - h, span, :] = blend(lambda i: dens[i, z - h, span, :]) + u[span, :]

    wide = ny + 2 * SUB
    inside = slice(SUB, SUB + ny)
    column = lax.broadcasted_iota(jnp.int32, (ny, nx), 1)
    place = column % h

    def plane_sum(d):
        total = pltpu.roll(d, h, 1) + pltpu.roll(d, nx - h, 1)
        return total + (pltpu.roll(d, 1, 0) + pltpu.roll(d, wide - 1, 0))

    all_of(2 * ny + 4 * count, xrecv).wait_recv()
    sub = lax.broadcasted_iota(jnp.int32, (SUB, nx), 0)
    for s in range(2):
        for end, (start, nearest) in enumerate(((0, SUB - 1), (ny + SUB, 0))):
            found = blend(lambda i: jnp.broadcast_to(cland[s, end, i:i + 1, :], (SUB, nx)))
            land[s, start:start + SUB, :] = jnp.where(
                sub == nearest, found, pltpu.roll(found, turn[s], 1)
            )

    sides = []
    for s in range(2):
        own = pack[1 - s]
        d = land[s] - jnp.concatenate([own[ny - SUB:], own, own[:SUB]], axis=0)
        m = plane_sum(d)
        mm = plane_sum(m)
        a1, a2 = by_distance(d[inside], m[inside], mm[inside])
        a3 = c3 * d[inside]
        if s == 0:
            a1, a2, a3 = (pltpu.roll(a, k + 1, 1) for k, a in enumerate((a1, a2, a3)))
            depth = place
        else:
            a1, a2, a3 = (pltpu.roll(a, nx - k - 1, 1) for k, a in enumerate((a1, a2, a3)))
            depth = (h - 1) - place
        sides.append(
            jnp.where(depth == 0, a1, 0.0) + jnp.where(depth <= 1, a2, 0.0) + a3
        )
    even = (column // h) % 2 == 0
    xc[0] = jnp.where(even, sides[1], sides[0])
    xc[1] = jnp.where(even, sides[0], sides[1])

    edge = (lane < h) | (lane >= nx - h)
    for z in range(nz):
        e = z + h
        for t in range(tiles):
            span = slice(t * SUB, (t + 1) * SUB)
            v = pltpu.roll(xc[e % 2, span, :], (-(h * e + h)) % nx, 1)
            base[z, span, :] = base[z, span, :] + jnp.where(edge, v, 0.0)

    all_of(2 * message_rows, yrecv).wait_recv()
    for q in range(h):
        rows = slice(q * nz, (q + 1) * nz)
        for s, p in enumerate((q, 2 * SUB - h + q)):
            yc[p * zp:p * zp + nz, :] = yland[s, rows, :] - ybuf[1 - s, rows, :]

    rows = total_devices - 1 + 2 * count * h * ny + 4 * count + 2 * ny + message_rows

    @pl.when(odd)
    def _():
        all_of(rows + 2 * message_rows, sent).wait_send()

    @pl.when(jnp.logical_not(odd))
    def _():
        all_of(rows + mate_rows, sent).wait_send()


def finish(base, yc, weights, out, wout, stage, sem, wsem):
    nz, ny, nx = base.shape
    zp = yc.shape[0] // (2 * SUB)
    pieces = 4
    per = nz // pieces

    def store(source, target):
        pltpu.make_async_copy(source, target, sem).start()

    wcopy = pltpu.make_async_copy(weights, wout, wsem)
    wcopy.start()
    if ny > 2 * SUB:
        middle = pl.ds(SUB, ny - 2 * SUB)
        store(base.at[:, middle], out.at[:, middle])
    for c in range(pieces):
        part = pl.ds(c * per, per)
        for k, start in enumerate((0, ny - SUB)):
            for z in range(c * per, (c + 1) * per):
                stage[k, z] = base[z, start:start + SUB, :] + yc[
                    pl.ds(k * SUB * zp + z, SUB, stride=zp), :
                ]
            store(stage.at[k, part], out.at[part, pl.ds(start, SUB)])
    pltpu.make_async_copy(base, out, sem).wait()
    wcopy.wait()


def on_device(counts, densities, residuals):
    dims = residuals.shape
    count, nz, ny, nx = dims
    h = SWEEPS
    ze = nz + 2 * h
    zp = pl.cdiv(ze, SUB) * SUB
    n = counts[0] * counts[1] * counts[2]
    chunks = [nz // 8] * 8
    tiles = ny // SUB
    assert tiles >= 2 and h * (ze + 1) <= nx and nz % 8 == 0 and counts[2] % 2 == 0
    dma = pltpu.SemaphoreType.DMA
    f32 = jnp.float32
    field = pltpu.VMEM((ze, ny, nx), f32)

    any_spec = pl.BlockSpec(memory_space=pl.ANY)
    vmem = pl.BlockSpec(memory_space=pltpu.VMEM)
    parts = pl.pallas_call(
        functools.partial(kernel, counts, dims, chunks),
        out_shape=(
            pltpu.VMEM((nz, ny, nx), f32),
            pltpu.VMEM((2 * SUB * zp, nx), f32),
            pltpu.VMEM((1, count), f32),
        ),
        in_specs=[any_spec, any_spec],
        out_specs=(vmem, vmem, vmem),
        scratch_shapes=[
            pltpu.VMEM((count, ze, ny, nx), f32),
            pltpu.VMEM(dims, f32),
            pltpu.VMEM((n, 1, nx), f32),
            field, field, field,
            pltpu.VMEM((count, 2, ny, nx), f32),
            pltpu.VMEM((2, ny, nx), f32),
            pltpu.VMEM((2, ny + 2 * SUB, nx), f32),
            pltpu.VMEM((2, 2, count, nx), f32),
            pltpu.VMEM((2, 2, count, nx), f32),
            pltpu.VMEM((count, 2 * SUB * zp, nx), f32),
            pltpu.VMEM((2, count, h * nz, nx), f32),
            pltpu.VMEM((count, h * nz, nx), f32),
            pltpu.VMEM((h * nz, nx), f32),
            pltpu.VMEM((2, h * nz, nx), f32),
            pltpu.VMEM((2, h * nz, nx), f32),
            pltpu.VMEM((2, ny, nx), f32),
            dma((len(chunks),)), *(dma(()) for _ in range(7)),
        ],
        compiler_params=pltpu.CompilerParams(
            collective_id=0, has_side_effects=True, vmem_limit_bytes=56 * 1024 * 1024
        ),
    )(residuals, densities)
    new_density, weights = pl.pallas_call(
        finish,
        out_shape=(
            jax.ShapeDtypeStruct((nz, ny, nx), f32),
            jax.ShapeDtypeStruct((1, count), f32),
        ),
        in_specs=[vmem, vmem, vmem],
        out_specs=(any_spec, any_spec),
        scratch_shapes=[pltpu.VMEM((2, nz, SUB, nx), f32), dma(()), dma(())],
        compiler_params=pltpu.CompilerParams(vmem_limit_bytes=4 * 1024 * 1024),
    )(*parts)
    return new_density, weights.reshape(count)


def solution(mesh):
    counts = tuple(mesh.shape[a] for a in AXES)
    placed = (P(None, "gz", "gy", "gx"), P(None, "gz", "gy", "gx"))
    return jax.shard_map(
        functools.partial(on_device, counts),
        mesh=mesh,
        in_specs=placed,
        out_specs=(P("gz", "gy", "gx"), P()),
        check_vma=False,
    )
```
